128 devices in a mesh: node: 32 (over x_hi, z, y), shard: 4 (over x_lo, core).
Axes of the slice: x: 4 (x_hi: 2, x_lo: 2; x = x_hi * 2 + x_lo), y: 4, z: 4, core: 2. Of those that a mesh axis runs over, the one named last changes fastest.
Arguments:
- inputs: bfloat16 [32, 1024, 1152], P('node', 'shard'), may hold values from -6 to 6
- upstream: bfloat16 [32, 1024, 1152], P('node', 'shard'), may hold values from -6 to 6
- counts: int32 [32], P('node'), may hold values from 1 to 4
- round_index: int32 [1], replicated, may hold values from 0 to 999
- rates: float32 [32], P('node'), may hold values from 0.002 to 0.008
- gate_weight: bfloat16 [32, 1152, 4608], P('node', None, 'shard'), may hold values from -0.1875 to 0.1875
- up_weight: bfloat16 [32, 1152, 4608], P('node', None, 'shard'), may hold values from -0.1875 to 0.1875
- down_weight: bfloat16 [32, 4608, 1152], P('node', 'shard'), may hold values from -0.09375 to 0.09375
Outputs:
- gate_mixed: bfloat16 [32, 1152, 4608], P('node', None, 'shard')
- up_mixed: bfloat16 [32, 1152, 4608], P('node', None, 'shard')
- down_mixed: bfloat16 [32, 4608, 1152], P('node', 'shard')
The draws below stay inside these ranges and needn't reach their ends.
Inputs may be any that keep to these rules, and one draw needn't show every extreme that they name: A node's live sequences fill its first counts slots of 4.
All inputs are finite; a program needn't handle non-finite values.
Results may differ from the reference program's by a relative error of at most 0.007.
Values may be sent and summed in bfloat16 or wider, within the bound.
A program may use at most 128 MiB of HBM per device.

```python
import math
import jax
import jax.numpy as jnp
from jax import lax

D = 1152
FF = 4608
SEQ = 256
SLOTS = 4
ROWS = 1024
N_NODE = 32


def plant(values, stream_key, smallest, largest):
    index_at = [jax.random.randint(jax.random.fold_in(stream_key, axis), (), 0, length) for axis, length in enumerate(values.shape)]
    longest = values.shape.index(max(values.shape))
    next_to = index_at[:longest] + [(index_at[longest] + 1) % values.shape[longest]] + index_at[longest + 1:]
    return values.at[tuple(index_at)].set(smallest).at[tuple(next_to)].set(largest)


def block_levels(own_key, dims, shards, smallest, top_value):
    gain = 1.0
    for dim, blocks in shards:
        heights = jax.random.uniform(jax.random.fold_in(jax.random.fold_in(own_key, 6), dim), (blocks,), jnp.float32, smallest / len(shards), top_value / len(shards))
        gain = gain * jnp.repeat(jnp.exp(heights), dims[dim] // blocks).reshape((-1,) + (1,) * (len(dims) - 1 - dim))
    return gain


def gaussian(key, shape, width, reach, split=(), held_as=jnp.bfloat16):
    level = block_levels(key, shape, split, -0.22, 0.18) if split else 1.0
    entries = jax.random.normal(key, shape, jnp.float32) * width * level
    return jnp.minimum(jnp.maximum(entries, -reach), reach).astype(held_as)


def setup_inputs(seed: int = 0) -> dict:
    splits = jax.random.split(jax.random.key(seed), 9)
    inputs = gaussian(splits[0], (N_NODE, ROWS, D), 1.0, 6.0, ((0, 32), (1, 4)))
    upstream = gaussian(splits[1], (N_NODE, ROWS, D), 1.0, 6.0, ((0, 32), (1, 4)))
    counts = plant(jax.random.randint(splits[2], (N_NODE,), 1, SLOTS + 1), jax.random.fold_in(splits[2], 1), 1, SLOTS).astype(jnp.int32)
    round_index = jax.random.randint(splits[3], (1,), 0, 1000).astype(jnp.int32)
    rates = jnp.clip(jnp.exp(math.log(0.008) - 1.3862944 * jax.random.uniform(splits[4], (N_NODE,), jnp.float32) ** block_levels(splits[4], (N_NODE,), ((0, 32),), -0.2, 0.2)), 0.002, 0.008)
    gate_weight = gaussian(splits[5], (N_NODE, D, FF), D ** -0.5, 0.1875, ((0, 32), (2, 4)))
    up_weight = gaussian(splits[6], (N_NODE, D, FF), D ** -0.5, 0.1875, ((0, 32), (2, 4)))
    down_weight = gaussian(splits[7], (N_NODE, FF, D), FF ** -0.5, 0.09375, ((0, 32), (1, 4)))
    return dict(inputs=inputs, upstream=upstream, counts=counts, round_index=round_index, rates=rates, gate_weight=gate_weight, up_weight=up_weight, down_weight=down_weight)


def gelu_tanh(values):
    return jax.nn.gelu(values, approximate=True)

def slot_grads(rows, grad_out, w_gate, w_up, w_down):
    floats = rows.astype(jnp.float32)
    normed = (floats * lax.rsqrt(lax.optimization_barrier(jnp.mean(floats * floats, -1, keepdims=True)) + 1e-06)).astype(jnp.bfloat16)
    pre_gate = jnp.dot(normed, w_gate, preferred_element_type=jnp.float32)
    pre_up = jnp.dot(normed, w_up, preferred_element_type=jnp.float32)
    act, pull = jax.vjp(gelu_tanh, pre_gate)
    slope = pull(jnp.ones_like(pre_gate))[0]
    hidden = (act * pre_up).astype(jnp.bfloat16)
    back = lax.dot_general(grad_out, w_down, (((1,), (1,)), ((), ())), preferred_element_type=jnp.float32)
    d_gate = (back * pre_up * slope).astype(jnp.bfloat16)
    d_up = (back * act).astype(jnp.bfloat16)
    inner = (((0,), (0,)), ((), ()))
    grad_gate = lax.dot_general(normed, d_gate, inner, preferred_element_type=jnp.float32)
    grad_up = lax.dot_general(normed, d_up, inner, preferred_element_type=jnp.float32)
    grad_down = lax.dot_general(hidden, grad_out, inner, preferred_element_type=jnp.float32)
    return (grad_gate, grad_up, grad_down)

def reference(inputs, upstream, counts, round_index, rates, gate_weight, up_weight, down_weight):
    levels = N_NODE.bit_length() - 1
    row_slot = (jnp.arange(SLOTS * SEQ, dtype=jnp.int32) // SEQ).astype(jnp.int32)
    decay = 250.0 / (250.0 + round_index[0].astype(jnp.float32))

    def one_node(items):
        rows, grads, count, rate, w_gate, w_up, w_down = items
        live = (row_slot < count)[:, None]
        grad_out = jnp.where(live, grads, jnp.zeros_like(grads))
        grad_gate, grad_up, grad_down = slot_grads(rows, grad_out, w_gate, w_up, w_down)
        step_size = rate * decay
        new_gate = (w_gate.astype(jnp.float32) - step_size * grad_gate).astype(jnp.bfloat16)
        new_up = (w_up.astype(jnp.float32) - step_size * grad_up).astype(jnp.bfloat16)
        new_down = (w_down.astype(jnp.float32) - step_size * grad_down).astype(jnp.bfloat16)
        return (new_gate, new_up, new_down)
    updated = lax.map(one_node, (inputs, upstream, counts, rates, gate_weight, up_weight, down_weight))
    which = (round_index[0] % levels).astype(jnp.int32)
    nodes = jnp.arange(N_NODE, dtype=jnp.int32)
    partners = jnp.bitwise_xor(nodes, jnp.left_shift(jnp.ones_like(nodes), which)).astype(jnp.int32)

    def mix_node(index):
        partner = partners[index]
        result = []
        for stacked in updated:
            mine = stacked[index].astype(jnp.float32)
            theirs = stacked[partner].astype(jnp.float32)
            result.append((0.5 * (mine + theirs)).astype(jnp.bfloat16))
        return tuple(result)
    mixed = lax.map(mix_node, nodes)
    return (mixed[0], mixed[1], mixed[2])
```

```python
import functools

import jax
import jax.numpy as jnp
from jax import lax
from jax.experimental import pallas as pl
from jax.experimental.pallas import tpu as pltpu
from jax.sharding import PartitionSpec as P

MESH = pl.DeviceIdType.MESH
CHUNK = 128
PIECES = 4
BLOCK = 128


def remote(src, dst, send_sem, recv_sem, device):
    return pltpu.make_async_remote_copy(
        src_ref=src,
        dst_ref=dst,
        send_sem=send_sem,
        recv_sem=recv_sem,
        device_id=device,
        device_id_type=MESH,
    )


def round_kernel(
    level,
    count_ref,
    step_ref,
    x_hbm,
    g_hbm,
    wg_hbm,
    wu_hbm,
    wd_hbm,
    mixed_gate,
    mixed_up,
    mixed_down,
    raw,
    normed,
    normed_t,
    grad_out,
    w_gate,
    w_up,
    w_down,
    d_both,
    hidden,
    own_gate,
    own_up,
    own_down,
    got_gate,
    got_up,
    got_down,
    local_sem,
    near_send,
    near_recv,
    far_send,
    far_recv,
    relay_send,
    relay_recv,
    chunk_send,
    chunk_recv,
    out_sem,
):
    node, shard = lax.axis_index("node"), lax.axis_index("shard")
    core, chip = lax.rem(shard, 2), shard // 2
    near = (node, chip * 2 + 1 - core)
    far = (node, (1 - chip) * 2 + core)
    stride = 1 << level
    peer = (node + (1 - 2 * lax.rem(node // stride, 2)) * stride, shard)
    seq = raw.shape[2]
    rows, width = normed.shape
    piece = seq // PIECES
    n_chunks = own_gate.shape[0]

    def load(i, src, dst):
        return pltpu.make_async_copy(src, dst, local_sem.at[i])

    loads = [
        load(0, x_hbm, raw.at[0, 0]),
        load(1, g_hbm, raw.at[1, 0]),
        load(2, wg_hbm, w_gate),
        load(3, wu_hbm, w_up),
        load(4, wd_hbm, w_down),
    ]
    for copy in loads:
        copy.start()

    barrier = pltpu.get_barrier_semaphore()
    for device in (near, far, peer):
        pl.semaphore_signal(barrier, inc=1, device_id=device, device_id_type=MESH)
    pl.semaphore_wait(barrier, 3)

    def to_far(kind, i):
        at = pl.ds(i * piece, piece)
        return remote(
            raw.at[kind, 0, at], raw.at[kind, 2, at], far_send.at[kind, i], far_recv.at[kind, i], far
        )

    def to_near(kind, i):
        at = pl.ds(i * piece, piece)
        return remote(
            raw.at[kind, 0, at], raw.at[kind, 1, at], near_send.at[kind, i], near_recv.at[kind, i], near
        )

    def relay(kind, i):
        at = pl.ds(i * piece, piece)
        return remote(
            raw.at[kind, 2, at], raw.at[kind, 3, at], relay_send.at[kind, i], relay_recv.at[kind, i], near
        )

    both = [(kind, i) for i in range(PIECES) for kind in range(2)]
    loads[0].wait()
    loads[1].wait()
    for kind, i in both:
        to_far(kind, i).start()
    for kind, i in both:
        to_near(kind, i).start()

    def prepare(slot, start):
        at = pl.ds(start, BLOCK)
        to = pl.ds(pl.multiple_of(slot * seq + start, BLOCK), BLOCK)
        floats = raw[0, slot, at].astype(jnp.float32)
        scale = lax.rsqrt(jnp.mean(floats * floats, -1, keepdims=True) + 1e-06)
        value = (floats * scale).astype(jnp.bfloat16)
        normed[to] = value
        normed_t[:, to] = value.T
        live = jnp.where(lax.bitwise_xor(shard, slot) < count_ref[0], 1.0, 0.0)
        grad_out[to] = (raw[1, slot, at].astype(jnp.float32) * live).astype(jnp.bfloat16)

    def prepare_slot(slot):
        @pl.loop(0, seq // BLOCK)
        def _(i):
            prepare(slot, pl.multiple_of(i * BLOCK, BLOCK))

    prepare_slot(0)
    for kind, i in both:
        to_near(kind, i).wait_recv()
    prepare_slot(1)
    for kind, i in both:
        to_far(kind, i).wait_recv()
        relay(kind, i).start()
    prepare_slot(2)
    for kind, i in both:
        relay(kind, i).wait_recv()
    prepare_slot(3)
    for copy in loads[2:]:
        copy.wait()

    step = step_ref[0]
    third = width // 3

    def sends(c):
        return [
            remote(mine.at[c], theirs.at[c], chunk_send.at[k, c], chunk_recv.at[k, c], peer)
            for k, (mine, theirs) in enumerate(
                ((own_gate, got_gate), (own_up, got_up), (own_down, got_down))
            )
        ]

    @pl.loop(0, n_chunks)
    def _(c):
        units = pl.ds(pl.multiple_of(c * CHUNK, CHUNK), CHUNK)

        @pl.loop(0, rows // seq)
        def _(r):
            at = pl.ds(pl.multiple_of(r * seq, seq), seq)
            n = normed[at]
            gate = jnp.dot(n, w_gate[:, units], preferred_element_type=jnp.float32)
            up = jnp.dot(n, w_up[:, units], preferred_element_type=jnp.float32)
            back = lax.dot_general(
                grad_out[at],
                w_down[units],
                (((1,), (1,)), ((), ())),
                preferred_element_type=jnp.float32,
            )
            k = 0.7978845608028654
            square = gate * gate
            t = jnp.tanh(gate * (k + (k * 0.044715) * square))
            half = 0.5 + 0.5 * t
            act = gate * half
            slope = half + (0.5 * gate) * (1.0 - t * t) * (k + (3.0 * k * 0.044715) * square)
            hidden[at] = (act * up).astype(jnp.bfloat16)
            d_both[at, :CHUNK] = (back * up * slope).astype(jnp.bfloat16)
            d_both[at, CHUNK:] = (back * act).astype(jnp.bfloat16)

        @pl.loop(0, 3)
        def _(b):
            at = pl.ds(pl.multiple_of(b * third, third), third)
            grad = jnp.dot(normed_t[at], d_both[...], preferred_element_type=jnp.float32)
            own_gate[c, at] = (
                w_gate[at, units].astype(jnp.float32) - step * grad[:, :CHUNK]
            ).astype(jnp.bfloat16)
            own_up[c, at] = (
                w_up[at, units].astype(jnp.float32) - step * grad[:, CHUNK:]
            ).astype(jnp.bfloat16)

        hidden_t = hidden[...].T

        @pl.loop(0, 3)
        def _(b):
            at = pl.ds(pl.multiple_of(b * third, third), third)
            grad = jnp.dot(hidden_t, grad_out[:, at], preferred_element_type=jnp.float32)
            own_down[c, :, at] = (
                w_down[units, at].astype(jnp.float32) - step * grad
            ).astype(jnp.bfloat16)

        for copy in sends(c):
            copy.start()

    def writes(c):
        units = pl.ds(pl.multiple_of(c * CHUNK, CHUNK), CHUNK)
        return [
            pltpu.make_async_copy(got_gate.at[c], mixed_gate.at[:, units], out_sem.at[0, c]),
            pltpu.make_async_copy(got_up.at[c], mixed_up.at[:, units], out_sem.at[1, c]),
            pltpu.make_async_copy(got_down.at[c], mixed_down.at[units], out_sem.at[2, c]),
        ]

    def average(mine, theirs):
        theirs[...] = (
            0.5 * (mine[...].astype(jnp.float32) + theirs[...].astype(jnp.float32))
        ).astype(jnp.bfloat16)

    @pl.loop(0, n_chunks)
    def _(c):
        for copy, write, mine, theirs in zip(
            sends(c),
            writes(c),
            (own_gate, own_up, own_down),
            (got_gate, got_up, got_down),
        ):
            copy.wait_recv()
            average(mine.at[c], theirs.at[c])
            write.start()

    @pl.loop(0, n_chunks)
    def _(c):
        for copy, write in zip(sends(c), writes(c)):
            copy.wait_send()
            write.wait()

    for kind, i in both:
        to_far(kind, i).wait_send()
        to_near(kind, i).wait_send()
        relay(kind, i).wait_send()


def one_level(level, count, step, x, g, w_gate, w_up, w_down):
    seq, width = x.shape
    units = w_gate.shape[1]
    n_chunks, rows = units // CHUNK, 4 * seq
    bf16 = jnp.bfloat16
    hbm = pl.BlockSpec(memory_space=pltpu.HBM)
    smem = pl.BlockSpec(memory_space=pltpu.SMEM)
    dma = pltpu.SemaphoreType.DMA
    across = pltpu.VMEM((n_chunks, width, CHUNK), bf16)
    along = pltpu.VMEM((n_chunks, CHUNK, width), bf16)
    return pl.pallas_call(
        functools.partial(round_kernel, level),
        out_shape=[jax.ShapeDtypeStruct(w.shape, bf16) for w in (w_gate, w_up, w_down)],
        in_specs=[smem, smem] + [hbm] * 5,
        out_specs=[hbm] * 3,
        scratch_shapes=[
            pltpu.VMEM((2, 4, seq, width), bf16),
            pltpu.VMEM((rows, width), bf16),
            pltpu.VMEM((width, rows), bf16),
            pltpu.VMEM((rows, width), bf16),
            pltpu.VMEM(w_gate.shape, bf16),
            pltpu.VMEM(w_up.shape, bf16),
            pltpu.VMEM(w_down.shape, bf16),
            pltpu.VMEM((rows, 2 * CHUNK), bf16),
            pltpu.VMEM((rows, CHUNK), bf16),
            across,
            across,
            along,
            across,
            across,
            along,
            dma((5,)),
            dma((2, PIECES)),
            dma((2, PIECES)),
            dma((2, PIECES)),
            dma((2, PIECES)),
            dma((2, PIECES)),
            dma((2, PIECES)),
            dma((3, n_chunks)),
            dma((3, n_chunks)),
            dma((3, n_chunks)),
        ],
        compiler_params=pltpu.CompilerParams(
            collective_id=level, has_side_effects=True, vmem_limit_bytes=56 << 20
        ),
        cost_estimate=pl.CostEstimate(
            flops=12 * rows * width * units,
            bytes_accessed=2 * (6 * width * units + 2 * seq * width),
            transcendentals=rows * units,
        ),
        name=f"round_level_{level}",
    )(count, step, x, g, w_gate, w_up, w_down)


def per_device(inputs, upstream, counts, round_index, rates, gate_weight, up_weight, down_weight):
    step = rates * (250.0 / (250.0 + round_index.astype(jnp.float32)))
    levels = lax.axis_size("node").bit_length() - 1
    mixed = lax.switch(
        round_index[0] % levels,
        [functools.partial(one_level, level) for level in range(levels)],
        counts,
        step,
        inputs[0],
        upstream[0],
        gate_weight[0],
        up_weight[0],
        down_weight[0],
    )
    return tuple(m[None] for m in mixed)


def solution(mesh):
    return jax.shard_map(
        per_device,
        mesh=mesh,
        in_specs=(
            P("node", "shard", None),
            P("node", "shard", None),
            P("node"),
            P(),
            P("node"),
            P("node", None, "shard"),
            P("node", None, "shard"),
            P("node", "shard", None),
        ),
        out_specs=(P("node", None, "shard"), P("node", None, "shard"), P("node", "shard", None)),
        check_vma=False,
    )
```

```python
import functools

import jax
import jax.numpy as jnp
from jax import lax
from jax.experimental import pallas as pl
from jax.experimental.pallas import tpu as pltpu
from jax.sharding import PartitionSpec as P

MESH = pl.DeviceIdType.MESH
CHUNK = 128
BLOCK = 128
PARTS = 3


def remote(src, dst, send_sem, recv_sem, device):
    return pltpu.make_async_remote_copy(
        src_ref=src,
        dst_ref=dst,
        send_sem=send_sem,
        recv_sem=recv_sem,
        device_id=device,
        device_id_type=MESH,
    )


def round_kernel(
    level,
    count_hbm,
    round_hbm,
    rate_hbm,
    x_hbm,
    g_hbm,
    wg_hbm,
    wu_hbm,
    wd_hbm,
    mixed_gate,
    mixed_up,
    mixed_down,
    raw,
    normed,
    normed_t,
    grad_out,
    w_gate,
    w_up,
    w_down,
    d_both,
    hidden,
    own_gate,
    own_up,
    own_down,
    got_gate,
    got_up,
    got_down,
    count_ref,
    round_ref,
    rate_ref,
    local_sem,
    near_send,
    near_recv,
    far_send,
    far_recv,
    relay_send,
    relay_recv,
    chunk_send,
    chunk_recv,
):
    node, shard = lax.axis_index("node"), lax.axis_index("shard")
    core, chip = lax.rem(shard, 2), shard // 2
    near = (node, chip * 2 + 1 - core)
    far = (node, (1 - chip) * 2 + core)
    stride = 1 << level
    peer = (node + (1 - 2 * lax.rem(node // stride, 2)) * stride, shard)
    n_blocks = raw.shape[1]
    width = normed.shape[1]
    n_chunks = own_gate.shape[0]

    def load(i, src, dst):
        return pltpu.make_async_copy(src, dst, local_sem.at[i])

    def rows_of(h):
        return pl.ds(h * BLOCK, BLOCK)

    slot_loads = [
        load(kind * 2 + h, src.at[rows_of(h)], raw.at[kind, h])
        for h in range(2)
        for kind, src in enumerate((x_hbm, g_hbm))
    ]
    other_loads = [
        load(4, wg_hbm, w_gate),
        load(5, wu_hbm, w_up),
        load(6, wd_hbm, w_down),
        load(7, count_hbm, count_ref),
        load(8, round_hbm, round_ref),
        load(9, rate_hbm, rate_ref),
    ]
    for copy in slot_loads + other_loads:
        copy.start()

    barrier = pltpu.get_barrier_semaphore()
    for device in (near, far, peer):
        pl.semaphore_signal(barrier, inc=1, device_id=device, device_id_type=MESH)
    pl.semaphore_wait(barrier, 3)

    def to_near(kind, h):
        return remote(
            raw.at[kind, h], raw.at[kind, 2 + h], near_send.at[kind, h], near_recv.at[kind, h], near
        )

    def to_far(kind, h):
        return remote(
            raw.at[kind, h], raw.at[kind, 4 + 2 * h], far_send.at[kind, h], far_recv.at[kind, h], far
        )

    def relay(kind, h):
        return remote(
            raw.at[kind, 4 + 2 * h],
            raw.at[kind, 5 + 2 * h],
            relay_send.at[kind, h],
            relay_recv.at[kind, h],
            near,
        )

    both = [(kind, h) for h in range(2) for kind in range(2)]
    for copy, (kind, h) in zip(slot_loads, both):
        copy.wait()
        to_far(kind, h).start()
    for kind, h in both:
        to_near(kind, h).start()
    for copy in other_loads:
        copy.wait()

    decay = 250.0 / (250.0 + jnp.full((8, 128), round_ref[0], jnp.int32).astype(jnp.float32))
    step = jnp.max(rate_ref[0] * decay)

    def prepare(block):
        to = pl.ds(pl.multiple_of(block * BLOCK, BLOCK), BLOCK)
        floats = raw[0, block].astype(jnp.float32)
        scale = lax.rsqrt(jnp.mean(floats * floats, -1, keepdims=True) + 1e-06)
        value = (floats * scale).astype(jnp.bfloat16)
        normed[to] = value
        normed_t[:, to] = value.T
        slot = lax.bitwise_xor(shard, jnp.where(block < 4, block // 2, 2 + lax.rem(block, 2)))
        live = jnp.where(slot < count_ref[0], 1.0, 0.0)
        grad_out[to] = (raw[1, block].astype(jnp.float32) * live).astype(jnp.bfloat16)

    def units_of(c):
        return pl.ds(pl.multiple_of(c * CHUNK, CHUNK), CHUNK)

    def forward(c, block):
        units = units_of(c)
        at = pl.ds(pl.multiple_of(block * BLOCK, BLOCK), BLOCK)
        n = normed[at]
        gate = jnp.dot(n, w_gate[:, units], preferred_element_type=jnp.float32)
        up = jnp.dot(n, w_up[:, units], preferred_element_type=jnp.float32)
        back = lax.dot_general(
            grad_out[at],
            w_down[units],
            (((1,), (1,)), ((), ())),
            preferred_element_type=jnp.float32,
        )
        k = 0.7978845608028654
        square = gate * gate
        t = jnp.tanh(gate * (k + (k * 0.044715) * square))
        half = 0.5 + 0.5 * t
        act = gate * half
        slope = half + (0.5 * gate) * (1.0 - t * t) * (k + (3.0 * k * 0.044715) * square)
        hidden[at] = (act * up).astype(jnp.bfloat16)
        d_both[at, :CHUNK] = (back * up * slope).astype(jnp.bfloat16)
        d_both[at, CHUNK:] = (back * act).astype(jnp.bfloat16)

    @pl.loop(0, n_blocks)
    def _(block):
        @pl.when(block == 2)
        def _():
            for kind, h in both:
                to_near(kind, h).wait_recv()

        @pl.when((block >= 4) & (lax.rem(block, 2) == 0))
        def _():
            h = block // 2 - 2
            for kind in range(2):
                to_far(kind, h).wait_recv()
                relay(kind, h).start()

        @pl.when((block >= 4) & (lax.rem(block, 2) == 1))
        def _():
            h = block // 2 - 2
            for kind in range(2):
                relay(kind, h).wait_recv()

        prepare(block)
        forward(0, block)

    part = width // PARTS
    pairs = ((own_gate, got_gate), (own_up, got_up), (own_down, got_down))

    def sent(k, c, at=None):
        mine, theirs = (ref.at[c] if at is None else ref.at[c, at] for ref in pairs[k])
        return remote(mine, theirs, chunk_send.at[k, c], chunk_recv.at[k, c], peer)

    @pl.loop(0, n_chunks)
    def _(c):
        units = units_of(c)

        @pl.loop(0, PARTS)
        def _(b):
            at = pl.ds(pl.multiple_of(b * part, part), part)
            grad = jnp.dot(normed_t[at], d_both[...], preferred_element_type=jnp.float32)
            own_gate[c, at] = (
                w_gate[at, units].astype(jnp.float32) - step * grad[:, :CHUNK]
            ).astype(jnp.bfloat16)
            own_up[c, at] = (
                w_up[at, units].astype(jnp.float32) - step * grad[:, CHUNK:]
            ).astype(jnp.bfloat16)
            sent(0, c, at).start()
            sent(1, c, at).start()

        hidden_t = hidden[...].T

        @pl.loop(0, PARTS)
        def _(b):
            at = pl.ds(pl.multiple_of(b * part, part), part)
            grad = jnp.dot(hidden_t, grad_out[:, at], preferred_element_type=jnp.float32)
            own_down[c, :, at] = (
                w_down[units, at].astype(jnp.float32) - step * grad
            ).astype(jnp.bfloat16)

        sent(2, c).start()

        @pl.when(c < n_chunks - 1)
        def _():
            @pl.loop(0, n_blocks)
            def _(block):
                forward(c + 1, block)

    def average(mine, theirs):
        return (0.5 * (mine.astype(jnp.float32) + theirs.astype(jnp.float32))).astype(jnp.bfloat16)

    @pl.loop(0, n_chunks)
    def _(c):
        units = units_of(c)
        sent(0, c).wait_recv()
        mixed_gate[:, units] = average(own_gate[c], got_gate[c])
        sent(1, c).wait_recv()
        mixed_up[:, units] = average(own_up[c], got_up[c])
        sent(2, c).wait_recv()
        mixed_down[units] = average(own_down[c], got_down[c])

    @pl.loop(0, n_chunks)
    def _(c):
        for k in range(3):
            sent(k, c).wait_send()

    for kind, h in both:
        to_far(kind, h).wait_send()
        to_near(kind, h).wait_send()
        relay(kind, h).wait_send()


def one_level(level, count, round_index, rate, x, g, w_gate, w_up, w_down):
    seq, width = x.shape
    units = w_gate.shape[1]
    n_chunks, rows = units // CHUNK, 4 * seq
    bf16 = jnp.bfloat16
    hbm = pl.BlockSpec(memory_space=pltpu.HBM)
    vmem = pl.BlockSpec(memory_space=pltpu.VMEM)
    dma = pltpu.SemaphoreType.DMA
    across = pltpu.VMEM((n_chunks, width, CHUNK), bf16)
    along = pltpu.VMEM((n_chunks, CHUNK, width), bf16)
    mixed = pl.pallas_call(
        functools.partial(round_kernel, level),
        out_shape=[pltpu.VMEM(w.shape, bf16) for w in (w_gate, w_up, w_down)],
        in_specs=[hbm] * 8,
        out_specs=[vmem] * 3,
        scratch_shapes=[
            pltpu.VMEM((2, rows // BLOCK, BLOCK, width), bf16),
            pltpu.VMEM((rows, width), bf16),
            pltpu.VMEM((width, rows), bf16),
            pltpu.VMEM((rows, width), bf16),
            pltpu.VMEM(w_gate.shape, bf16),
            pltpu.VMEM(w_up.shape, bf16),
            pltpu.VMEM(w_down.shape, bf16),
            pltpu.VMEM((rows, 2 * CHUNK), bf16),
            pltpu.VMEM((rows, CHUNK), bf16),
            across,
            across,
            along,
            across,
            across,
            along,
            pltpu.SMEM((1,), jnp.int32),
            pltpu.SMEM((1,), jnp.int32),
            pltpu.SMEM((1,), jnp.float32),
            dma((10,)),
            dma((2, 2)),
            dma((2, 2)),
            dma((2, 2)),
            dma((2, 2)),
            dma((2, 2)),
            dma((2, 2)),
            dma((3, n_chunks)),
            dma((3, n_chunks)),
        ],
        compiler_params=pltpu.CompilerParams(
            collective_id=level, has_side_effects=True, vmem_limit_bytes=44 << 20
        ),
        cost_estimate=pl.CostEstimate(
            flops=12 * rows * width * units,
            bytes_accessed=2 * (6 * width * units + 2 * seq * width),
            transcendentals=rows * units,
        ),
        name=f"round_level_{level}",
    )(count, round_index, rate, x, g, w_gate, w_up, w_down)
    return write_out(*mixed)


def write_kernel(gate, up, down, out_gate, out_up, out_down, sem):
    copies = [
        pltpu.make_async_copy(src, dst, sem.at[i])
        for i, (src, dst) in enumerate(((gate, out_gate), (up, out_up), (down, out_down)))
    ]
    for copy in copies:
        copy.start()
    for copy in copies:
        copy.wait()


def write_out(*arrays):
    return pl.pallas_call(
        write_kernel,
        out_shape=[jax.ShapeDtypeStruct(a.shape, a.dtype) for a in arrays],
        in_specs=[pl.BlockSpec(memory_space=pltpu.VMEM)] * 3,
        out_specs=[pl.BlockSpec(memory_space=pltpu.HBM)] * 3,
        scratch_shapes=[pltpu.SemaphoreType.DMA((3,))],
        compiler_params=pltpu.CompilerParams(vmem_limit_bytes=16 << 20),
        name="write_out",
    )(*arrays)


def per_device(inputs, upstream, counts, round_index, rates, gate_weight, up_weight, down_weight):
    levels = lax.axis_size("node").bit_length() - 1
    mixed = lax.switch(
        lax.rem(round_index[0], levels),
        [functools.partial(one_level, level) for level in range(levels)],
        counts,
        round_index,
        rates,
        inputs[0],
        upstream[0],
        gate_weight[0],
        up_weight[0],
        down_weight[0],
    )
    return tuple(m[None] for m in mixed)


def solution(mesh):
    return jax.shard_map(
        per_device,
        mesh=mesh,
        in_specs=(
            P("node", "shard", None),
            P("node", "shard", None),
            P("node"),
            P(),
            P("node"),
            P("node", None, "shard"),
            P("node", None, "shard"),
            P("node", "shard", None),
        ),
        out_specs=(P("node", None, "shard"), P("node", None, "shard"), P("node", "shard", None)),
        check_vma=False,
    )
```

```python
import functools

import jax
import jax.numpy as jnp
from jax import lax
from jax.experimental import pallas as pl
from jax.experimental.pallas import tpu as pltpu
from jax.sharding import PartitionSpec as P

MESH = pl.DeviceIdType.MESH
CHUNK = 128
BLOCK = 128
PARTS = 3


def remote(src, dst, send_sem, recv_sem, device):
    return pltpu.make_async_remote_copy(
        src_ref=src,
        dst_ref=dst,
        send_sem=send_sem,
        recv_sem=recv_sem,
        device_id=device,
        device_id_type=MESH,
    )


def round_kernel(
    level,
    early,
    count_hbm,
    round_hbm,
    rate_hbm,
    x_hbm,
    g_hbm,
    wg_hbm,
    wu_hbm,
    wd_hbm,
    mixed_gate,
    mixed_up,
    mixed_down,
    raw,
    normed,
    normed_t,
    grad_out,
    w_gate,
    w_up,
    w_down,
    d_both,
    hidden,
    own_gate,
    own_up,
    own_down,
    got_gate,
    got_up,
    got_down,
    count_ref,
    round_ref,
    rate_ref,
    local_sem,
    near_send,
    near_recv,
    far_send,
    far_recv,
    relay_send,
    relay_recv,
    chunk_send,
    chunk_recv,
    *partner,
):
    node, shard = lax.axis_index("node"), lax.axis_index("shard")
    core, chip = lax.rem(shard, 2), shard // 2
    near = (node, chip * 2 + 1 - core)
    far = (node, (1 - chip) * 2 + core)
    stride = 1 << level
    peer = (node + (1 - 2 * lax.rem(node // stride, 2)) * stride, shard)
    n_blocks = raw.shape[1]
    width = normed.shape[1]
    n_chunks = own_gate.shape[0]

    def load(i, src, dst):
        return pltpu.make_async_copy(src, dst, local_sem.at[i])

    def rows_of(h):
        return pl.ds(h * BLOCK, BLOCK)

    slot_loads = [
        load(kind * 2 + h, src.at[rows_of(h)], raw.at[kind, h])
        for h in range(2)
        for kind, src in enumerate((x_hbm, g_hbm))
    ]
    other_loads = [
        load(4, wg_hbm, w_gate),
        load(5, wu_hbm, w_up),
        load(6, wd_hbm, w_down),
        load(7, count_hbm, count_ref),
        load(8, round_hbm, round_ref),
        load(9, rate_hbm, rate_ref),
    ]
    for copy in slot_loads + other_loads:
        copy.start()

    barrier = pltpu.get_barrier_semaphore()
    for device in (near, far, peer):
        pl.semaphore_signal(barrier, inc=1, device_id=device, device_id_type=MESH)
    pl.semaphore_wait(barrier, 3)

    def hop(sems, blocks, start, stop, device):
        def copy(kind, h):
            return remote(
                blocks.at[kind, start(h)],
                blocks.at[kind, stop(h)],
                sems[0].at[kind, h],
                sems[1].at[kind, h],
                device,
            )

        return copy

    def hops(near_sems, far_sems, relay_sems, blocks):
        return (
            hop(near_sems, blocks, lambda h: h, lambda h: 2 + h, near),
            hop(far_sems, blocks, lambda h: h, lambda h: 4 + 2 * h, far),
            hop(relay_sems, blocks, lambda h: 4 + 2 * h, lambda h: 5 + 2 * h, near),
        )

    to_near, to_far, relay = hops(
        (near_send, near_recv), (far_send, far_recv), (relay_send, relay_recv), raw
    )
    if early:
        (theirs, their_gate, their_up, their_down, scalars, their_scalars, *sems) = partner
        slot_sems, near_sems, far_sems, relay_sems, weight_sems, scalar_sems = (
            sems[i : i + 2] for i in range(0, 12, 2)
        )

        def to_peer(kind, h):
            return remote(
                raw.at[kind, h],
                theirs.at[kind, h],
                slot_sems[0].at[kind, h],
                slot_sems[1].at[kind, h],
                peer,
            )

        their_near, their_far, their_relay = hops(near_sems, far_sems, relay_sems, theirs)
        first = pl.ds(0, CHUNK)
        weight_copies = [
            remote(src, dst, weight_sems[0].at[k], weight_sems[1].at[k], peer)
            for k, (src, dst) in enumerate(
                (
                    (w_gate.at[:, first], their_gate),
                    (w_up.at[:, first], their_up),
                    (w_down.at[first], their_down),
                )
            )
        ]
        scalar_copy = remote(
            scalars, their_scalars, scalar_sems[0].at[0], scalar_sems[1].at[0], peer
        )

    both = [(kind, h) for h in range(2) for kind in range(2)]
    for copy, (kind, h) in zip(slot_loads, both):
        copy.wait()
        to_far(kind, h).start()
        if early:
            to_peer(kind, h).start()
    for kind, h in both:
        to_near(kind, h).start()
    for copy in other_loads:
        copy.wait()
    if early:
        for copy in weight_copies:
            copy.start()

    decay = 250.0 / (250.0 + jnp.full((8, 128), round_ref[0], jnp.int32).astype(jnp.float32))
    step = jnp.max(rate_ref[0] * decay)
    count = count_ref[0].astype(jnp.float32)
    if early:
        scalars[0] = rate_ref[0] * decay
        scalars[1] = jnp.full((8, 128), count, jnp.float32)

    def prepare(blocks, block, count):
        to = pl.ds(pl.multiple_of(block * BLOCK, BLOCK), BLOCK)
        floats = blocks[0, block].astype(jnp.float32)
        scale = lax.rsqrt(jnp.mean(floats * floats, -1, keepdims=True) + 1e-06)
        value = (floats * scale).astype(jnp.bfloat16)
        normed[to] = value
        normed_t[:, to] = value.T
        slot = lax.bitwise_xor(shard, jnp.where(block < 4, block // 2, 2 + lax.rem(block, 2)))
        live = jnp.where(slot.astype(jnp.float32) < count, 1.0, 0.0)
        grad_out[to] = (blocks[1, block].astype(jnp.float32) * live).astype(jnp.bfloat16)

    def units_of(c):
        return pl.ds(pl.multiple_of(c * CHUNK, CHUNK), CHUNK)

    def forward(gate_weight, up_weight, down_weight, block):
        at = pl.ds(pl.multiple_of(block * BLOCK, BLOCK), BLOCK)
        n = normed[at]
        gate = jnp.dot(n, gate_weight[...], preferred_element_type=jnp.float32)
        up = jnp.dot(n, up_weight[...], preferred_element_type=jnp.float32)
        back = lax.dot_general(
            grad_out[at],
            down_weight[...],
            (((1,), (1,)), ((), ())),
            preferred_element_type=jnp.float32,
        )
        k = 0.7978845608028654
        square = gate * gate
        t = jnp.tanh(gate * (k + (k * 0.044715) * square))
        half = 0.5 + 0.5 * t
        act = gate * half
        slope = half + (0.5 * gate) * (1.0 - t * t) * (k + (3.0 * k * 0.044715) * square)
        hidden[at] = (act * up).astype(jnp.bfloat16)
        d_both[at, :CHUNK] = (back * up * slope).astype(jnp.bfloat16)
        d_both[at, CHUNK:] = (back * act).astype(jnp.bfloat16)

    def own_weights(c):
        units = units_of(c)
        return w_gate.at[:, units], w_up.at[:, units], w_down.at[units]

    @pl.loop(0, n_blocks)
    def _(block):
        @pl.when(block == 2)
        def _():
            for kind, h in both:
                to_near(kind, h).wait_recv()

        @pl.when((block >= 4) & (lax.rem(block, 2) == 0))
        def _():
            h = block // 2 - 2
            for kind in range(2):
                to_far(kind, h).wait_recv()
                relay(kind, h).start()

        @pl.when((block >= 4) & (lax.rem(block, 2) == 1))
        def _():
            h = block // 2 - 2
            for kind in range(2):
                relay(kind, h).wait_recv()

        prepare(raw, block, count)
        forward(*own_weights(0), block)

    if early:
        scalar_copy.start()
        for kind, h in both:
            to_peer(kind, h).wait_recv()
            their_far(kind, h).start()
            their_near(kind, h).start()

    part = width // PARTS
    pairs = ((own_gate, got_gate), (own_up, got_up), (own_down, got_down))

    def sent(k, c, at=None):
        mine, theirs = (ref.at[c] if at is None else ref.at[c, at] for ref in pairs[k])
        return remote(mine, theirs, chunk_send.at[k, c], chunk_recv.at[k, c], peer)

    def update(weights, results, step, ready):
        gate_weight, up_weight, down_weight = weights
        gate_result, up_result, down_result = results

        @pl.loop(0, PARTS)
        def _(b):
            at = pl.ds(pl.multiple_of(b * part, part), part)
            grad = jnp.dot(normed_t[at], d_both[...], preferred_element_type=jnp.float32)
            gate_result[at] = (
                gate_weight[at].astype(jnp.float32) - step * grad[:, :CHUNK]
            ).astype(jnp.bfloat16)
            up_result[at] = (
                up_weight[at].astype(jnp.float32) - step * grad[:, CHUNK:]
            ).astype(jnp.bfloat16)
            ready(0, at)
            ready(1, at)

        hidden_t = hidden[...].T

        @pl.loop(0, PARTS)
        def _(b):
            at = pl.ds(pl.multiple_of(b * part, part), part)
            grad = jnp.dot(hidden_t, grad_out[:, at], preferred_element_type=jnp.float32)
            down_result[:, at] = (
                down_weight[:, at].astype(jnp.float32) - step * grad
            ).astype(jnp.bfloat16)

        ready(2, None)

    @pl.loop(0, n_chunks)
    def _(c):
        def send(k, at):
            if early:

                @pl.when(c > 0)
                def _():
                    sent(k, c, at).start()

            else:
                sent(k, c, at).start()

        update(
            own_weights(c), (own_gate.at[c], own_up.at[c], own_down.at[c]), step, send
        )

        @pl.when(c < n_chunks - 1)
        def _():
            @pl.loop(0, n_blocks)
            def _(block):
                forward(*own_weights(c + 1), block)

    if early:
        for kind, h in both:
            their_far(kind, h).wait_recv()
            their_relay(kind, h).start()
            their_near(kind, h).wait_recv()
        for copy in weight_copies:
            copy.wait_recv()
        scalar_copy.wait_recv()
        for kind, h in both:
            their_relay(kind, h).wait_recv()
        their_step = jnp.max(their_scalars[0])
        their_count = jnp.max(their_scalars[1])

        @pl.loop(0, n_blocks)
        def _(block):
            prepare(theirs, block, their_count)
            forward(their_gate, their_up, their_down, block)

        update(
            (their_gate, their_up, their_down),
            (got_gate.at[0], got_up.at[0], got_down.at[0]),
            their_step,
            lambda k, at: None,
        )

    def average(mine, theirs):
        return (0.5 * (mine.astype(jnp.float32) + theirs.astype(jnp.float32))).astype(jnp.bfloat16)

    @pl.loop(0, n_chunks)
    def _(c):
        units = units_of(c)

        def arrived(k):
            if early:

                @pl.when(c > 0)
                def _():
                    sent(k, c).wait_recv()

            else:
                sent(k, c).wait_recv()

        arrived(0)
        mixed_gate[:, units] = average(own_gate[c], got_gate[c])
        arrived(1)
        mixed_up[:, units] = average(own_up[c], got_up[c])
        arrived(2)
        mixed_down[units] = average(own_down[c], got_down[c])

    @pl.loop(1 if early else 0, n_chunks)
    def _(c):
        for k in range(3):
            sent(k, c).wait_send()

    gathers = [to_far, to_near, relay]
    if early:
        gathers += [to_peer, their_far, their_near, their_relay]
        for copy in weight_copies + [scalar_copy]:
            copy.wait_send()
    for kind, h in both:
        for copy in gathers:
            copy(kind, h).wait_send()


def one_level(level, early, count, round_index, rate, x, g, w_gate, w_up, w_down):
    seq, width = x.shape
    units = w_gate.shape[1]
    n_chunks, rows = units // CHUNK, 4 * seq
    bf16 = jnp.bfloat16
    hbm = pl.BlockSpec(memory_space=pltpu.HBM)
    vmem = pl.BlockSpec(memory_space=pltpu.VMEM)
    dma = pltpu.SemaphoreType.DMA
    across = pltpu.VMEM((n_chunks, width, CHUNK), bf16)
    along = pltpu.VMEM((n_chunks, CHUNK, width), bf16)
    raw = pltpu.VMEM((2, rows // BLOCK, BLOCK, width), bf16)
    partner = [
        raw,
        pltpu.VMEM((width, CHUNK), bf16),
        pltpu.VMEM((width, CHUNK), bf16),
        pltpu.VMEM((CHUNK, width), bf16),
        pltpu.VMEM((2, 8, 128), jnp.float32),
        pltpu.VMEM((2, 8, 128), jnp.float32),
    ]
    partner += [dma((2, 2))] * 8 + [dma((3,))] * 2 + [dma((1,))] * 2
    mixed = pl.pallas_call(
        functools.partial(round_kernel, level, early),
        out_shape=[pltpu.VMEM(w.shape, bf16) for w in (w_gate, w_up, w_down)],
        in_specs=[hbm] * 8,
        out_specs=[vmem] * 3,
        scratch_shapes=[
            raw,
            pltpu.VMEM((rows, width), bf16),
            pltpu.VMEM((width, rows), bf16),
            pltpu.VMEM((rows, width), bf16),
            pltpu.VMEM(w_gate.shape, bf16),
            pltpu.VMEM(w_up.shape, bf16),
            pltpu.VMEM(w_down.shape, bf16),
            pltpu.VMEM((rows, 2 * CHUNK), bf16),
            pltpu.VMEM((rows, CHUNK), bf16),
            across,
            across,
            along,
            across,
            across,
            along,
            pltpu.SMEM((1,), jnp.int32),
            pltpu.SMEM((1,), jnp.int32),
            pltpu.SMEM((1,), jnp.float32),
            dma((10,)),
            dma((2, 2)),
            dma((2, 2)),
            dma((2, 2)),
            dma((2, 2)),
            dma((2, 2)),
            dma((2, 2)),
            dma((3, n_chunks)),
            dma((3, n_chunks)),
            *(partner if early else ()),
        ],
        compiler_params=pltpu.CompilerParams(
            collective_id=level, has_side_effects=True, vmem_limit_bytes=44 << 20
        ),
        cost_estimate=pl.CostEstimate(
            flops=12 * rows * width * units,
            bytes_accessed=2 * (6 * width * units + 2 * seq * width),
            transcendentals=rows * units,
        ),
        name=f"round_level_{level}",
    )(count, round_index, rate, x, g, w_gate, w_up, w_down)
    return write_out(*mixed)


def write_kernel(gate, up, down, out_gate, out_up, out_down, sem):
    copies = [
        pltpu.make_async_copy(src, dst, sem.at[i])
        for i, (src, dst) in enumerate(((gate, out_gate), (up, out_up), (down, out_down)))
    ]
    for copy in copies:
        copy.start()
    for copy in copies:
        copy.wait()


def write_out(*arrays):
    return pl.pallas_call(
        write_kernel,
        out_shape=[jax.ShapeDtypeStruct(a.shape, a.dtype) for a in arrays],
        in_specs=[pl.BlockSpec(memory_space=pltpu.VMEM)] * 3,
        out_specs=[pl.BlockSpec(memory_space=pltpu.HBM)] * 3,
        scratch_shapes=[pltpu.SemaphoreType.DMA((3,))],
        compiler_params=pltpu.CompilerParams(vmem_limit_bytes=16 << 20),
        name="write_out",
    )(*arrays)


def per_device(inputs, upstream, counts, round_index, rates, gate_weight, up_weight, down_weight):
    levels = lax.axis_size("node").bit_length() - 1
    mixed = lax.switch(
        lax.rem(round_index[0], levels),
        [functools.partial(one_level, level, level < levels - 1) for level in range(levels)],
        counts,
        round_index,
        rates,
        inputs[0],
        upstream[0],
        gate_weight[0],
        up_weight[0],
        down_weight[0],
    )
    return tuple(m[None] for m in mixed)


def solution(mesh):
    return jax.shard_map(
        per_device,
        mesh=mesh,
        in_specs=(
            P("node", "shard", None),
            P("node", "shard", None),
            P("node"),
            P(),
            P("node"),
            P("node", None, "shard"),
            P("node", None, "shard"),
            P("node", "shard", None),
        ),
        out_specs=(P("node", None, "shard"), P("node", None, "shard"), P("node", "shard", None)),
        check_vma=False,
    )
```

```python
import functools

import jax
import jax.numpy as jnp
from jax import lax
from jax.experimental import pallas as pl
from jax.experimental.pallas import tpu as pltpu
from jax.sharding import PartitionSpec as P

MESH = pl.DeviceIdType.MESH
CHUNK = 128
BLOCK = 128
PARTS = 3


def remote(src, dst, send_sem, recv_sem, device):
    return pltpu.make_async_remote_copy(
        src_ref=src,
        dst_ref=dst,
        send_sem=send_sem,
        recv_sem=recv_sem,
        device_id=device,
        device_id_type=MESH,
    )


def round_kernel(
    level,
    early,
    count_hbm,
    round_hbm,
    rate_hbm,
    x_hbm,
    g_hbm,
    wg_hbm,
    wu_hbm,
    wd_hbm,
    mixed_gate,
    mixed_up,
    mixed_down,
    raw,
    normed,
    normed_t,
    grad_out,
    w_gate,
    w_up,
    w_down,
    d_both,
    hidden,
    own_gate,
    own_up,
    own_down,
    got_gate,
    got_up,
    got_down,
    count_ref,
    round_ref,
    rate_ref,
    local_sem,
    near_send,
    near_recv,
    far_send,
    far_recv,
    relay_send,
    relay_recv,
    chunk_send,
    chunk_recv,
    *partner,
):
    node, shard = lax.axis_index("node"), lax.axis_index("shard")
    core, chip = lax.rem(shard, 2), shard // 2
    near = (node, chip * 2 + 1 - core)
    far = (node, (1 - chip) * 2 + core)
    stride = 1 << level
    peer = (node + (1 - 2 * lax.rem(node // stride, 2)) * stride, shard)
    n_blocks = raw.shape[1]
    width = normed.shape[1]
    n_chunks = own_gate.shape[0]

    def load(i, src, dst):
        return pltpu.make_async_copy(src, dst, local_sem.at[i])

    def rows_of(h):
        return pl.ds(h * BLOCK, BLOCK)

    slot_loads = [
        load(kind * 2 + h, src.at[rows_of(h)], raw.at[kind, h])
        for h in range(2)
        for kind, src in enumerate((x_hbm, g_hbm))
    ]
    other_loads = [
        load(4, wg_hbm, w_gate),
        load(5, wu_hbm, w_up),
        load(6, wd_hbm, w_down),
        load(7, count_hbm, count_ref),
        load(8, round_hbm, round_ref),
        load(9, rate_hbm, rate_ref),
    ]
    for copy in slot_loads + other_loads:
        copy.start()

    barrier = pltpu.get_barrier_semaphore()
    for device in (near, far, peer):
        pl.semaphore_signal(barrier, inc=1, device_id=device, device_id_type=MESH)
    pl.semaphore_wait(barrier, 3)

    def hop(sems, blocks, start, stop, device):
        def copy(kind, h):
            return remote(
                blocks.at[kind, start(h)],
                blocks.at[kind, stop(h)],
                sems[0].at[kind, h],
                sems[1].at[kind, h],
                device,
            )

        return copy

    def hops(near_sems, far_sems, relay_sems, blocks):
        return (
            hop(near_sems, blocks, lambda h: h, lambda h: 2 + h, near),
            hop(far_sems, blocks, lambda h: h, lambda h: 4 + 2 * h, far),
            hop(relay_sems, blocks, lambda h: 4 + 2 * h, lambda h: 5 + 2 * h, near),
        )

    to_near, to_far, relay = hops(
        (near_send, near_recv), (far_send, far_recv), (relay_send, relay_recv), raw
    )
    if early:
        (theirs, their_gate, their_up, back_sent, their_back, scalars, their_scalars, *sems) = partner
        slot_sems, near_sems, far_sems, relay_sems, weight_sems, back_sems, scalar_sems = (
            sems[i : i + 2] for i in range(0, 14, 2)
        )

        def to_peer(h):
            return remote(
                raw.at[0, h], theirs.at[0, h], slot_sems[0].at[h], slot_sems[1].at[h], peer
            )

        def back_copy(block):
            return remote(
                back_sent.at[block],
                their_back.at[block],
                back_sems[0].at[block],
                back_sems[1].at[block],
                peer,
            )

        their_near, their_far, their_relay = hops(near_sems, far_sems, relay_sems, theirs)
        first = pl.ds(0, CHUNK)
        weight_copies = [
            remote(src, dst, weight_sems[0].at[k], weight_sems[1].at[k], peer)
            for k, (src, dst) in enumerate(
                ((w_gate.at[:, first], their_gate), (w_up.at[:, first], their_up))
            )
        ]
        scalar_copy = remote(
            scalars, their_scalars, scalar_sems[0].at[0], scalar_sems[1].at[0], peer
        )

    both = [(kind, h) for h in range(2) for kind in range(2)]
    for copy, (kind, h) in zip(slot_loads, both):
        copy.wait()
        to_far(kind, h).start()
        if early and kind == 0:
            to_peer(h).start()
    for kind, h in both:
        to_near(kind, h).start()
    for copy in other_loads:
        copy.wait()
    if early:
        for copy in weight_copies:
            copy.start()

    decay = 250.0 / (250.0 + jnp.full((8, 128), round_ref[0], jnp.int32).astype(jnp.float32))
    step = jnp.max(rate_ref[0] * decay)
    count = count_ref[0].astype(jnp.float32)
    if early:
        scalars[...] = rate_ref[0] * decay

    def prepare(blocks, block, count):
        to = pl.ds(pl.multiple_of(block * BLOCK, BLOCK), BLOCK)
        floats = blocks[0, block].astype(jnp.float32)
        scale = lax.rsqrt(jnp.mean(floats * floats, -1, keepdims=True) + 1e-06)
        value = (floats * scale).astype(jnp.bfloat16)
        normed[to] = value
        normed_t[:, to] = value.T
        if count is None:
            return
        slot = lax.bitwise_xor(shard, jnp.where(block < 4, block // 2, 2 + lax.rem(block, 2)))
        live = jnp.where(slot.astype(jnp.float32) < count, 1.0, 0.0)
        grad_out[to] = (blocks[1, block].astype(jnp.float32) * live).astype(jnp.bfloat16)

    def units_of(c):
        return pl.ds(pl.multiple_of(c * CHUNK, CHUNK), CHUNK)

    def forward(gate_weight, up_weight, block, back_of, outputs):
        at = pl.ds(pl.multiple_of(block * BLOCK, BLOCK), BLOCK)
        n = normed[at]
        gate = jnp.dot(n, gate_weight[...], preferred_element_type=jnp.float32)
        up = jnp.dot(n, up_weight[...], preferred_element_type=jnp.float32)
        back = back_of(at)
        k = 0.7978845608028654
        square = gate * gate
        t = jnp.tanh(gate * (k + (k * 0.044715) * square))
        half = 0.5 + 0.5 * t
        act = gate * half
        slope = half + (0.5 * gate) * (1.0 - t * t) * (k + (3.0 * k * 0.044715) * square)
        if outputs:
            hidden[at] = (act * up).astype(jnp.bfloat16)
        d_both[at, :CHUNK] = (back * up * slope).astype(jnp.bfloat16)
        d_both[at, CHUNK:] = (back * act).astype(jnp.bfloat16)

    def own_weights(c):
        units = units_of(c)
        return w_gate.at[:, units], w_up.at[:, units], w_down.at[units]

    def own_forward(c, block, keep_back=False):
        gate_weight, up_weight, down_weight = own_weights(c)

        def back_of(at):
            back = lax.dot_general(
                grad_out[at],
                down_weight[...],
                (((1,), (1,)), ((), ())),
                preferred_element_type=jnp.float32,
            )
            if keep_back:
                back_sent[block] = back.astype(jnp.bfloat16)
            return back

        forward(gate_weight, up_weight, block, back_of, True)

    @pl.loop(0, n_blocks)
    def _(block):
        @pl.when(block == 2)
        def _():
            for kind, h in both:
                to_near(kind, h).wait_recv()

        @pl.when((block >= 4) & (lax.rem(block, 2) == 0))
        def _():
            h = block // 2 - 2
            for kind in range(2):
                to_far(kind, h).wait_recv()
                relay(kind, h).start()

        @pl.when((block >= 4) & (lax.rem(block, 2) == 1))
        def _():
            h = block // 2 - 2
            for kind in range(2):
                relay(kind, h).wait_recv()

        prepare(raw, block, count)
        own_forward(0, block, keep_back=early)
        if early:
            back_copy(block).start()

    if early:
        scalar_copy.start()
        for h in range(2):
            to_peer(h).wait_recv()
            their_far(0, h).start()
            their_near(0, h).start()

    part = width // PARTS
    pairs = ((own_gate, got_gate), (own_up, got_up), (own_down, got_down))

    def sent(k, c, at=None):
        mine, theirs = (ref.at[c] if at is None else ref.at[c, at] for ref in pairs[k])
        return remote(mine, theirs, chunk_send.at[k, c], chunk_recv.at[k, c], peer)

    def update_across(weights, results, step, ready):
        gate_weight, up_weight = weights
        gate_result, up_result = results

        @pl.loop(0, PARTS)
        def _(b):
            at = pl.ds(pl.multiple_of(b * part, part), part)
            grad = jnp.dot(normed_t[at], d_both[...], preferred_element_type=jnp.float32)
            gate_result[at] = (
                gate_weight[at].astype(jnp.float32) - step * grad[:, :CHUNK]
            ).astype(jnp.bfloat16)
            up_result[at] = (
                up_weight[at].astype(jnp.float32) - step * grad[:, CHUNK:]
            ).astype(jnp.bfloat16)
            ready(at)

    def update_down(weight, result):
        hidden_t = hidden[...].T

        @pl.loop(0, PARTS)
        def _(b):
            at = pl.ds(pl.multiple_of(b * part, part), part)
            grad = jnp.dot(hidden_t, grad_out[:, at], preferred_element_type=jnp.float32)
            result[:, at] = (weight[:, at].astype(jnp.float32) - step * grad).astype(jnp.bfloat16)

    def across_travels(c, act):
        if early:
            pl.when(c > 0)(act)
        else:
            act()

    @pl.loop(0, n_chunks)
    def _(c):
        weights = own_weights(c)

        def send(at):
            def start():
                sent(0, c, at).start()
                sent(1, c, at).start()

            across_travels(c, start)

        def down():
            update_down(weights[2], own_down.at[c])
            sent(2, c).start()

        update_across(weights[:2], (own_gate.at[c], own_up.at[c]), step, send)
        down()

        @pl.when(c < n_chunks - 1)
        def _():
            @pl.loop(0, n_blocks)
            def _(block):
                own_forward(c + 1, block)

    if early:
        for h in range(2):
            their_far(0, h).wait_recv()
            their_relay(0, h).start()
            their_near(0, h).wait_recv()
        for copy in weight_copies:
            copy.wait_recv()
        scalar_copy.wait_recv()
        for h in range(2):
            their_relay(0, h).wait_recv()
        their_step = jnp.max(their_scalars[...])

        @pl.loop(0, n_blocks)
        def _(block):
            prepare(theirs, block, None)
            back_copy(block).wait_recv()
            forward(
                their_gate,
                their_up,
                block,
                lambda at: their_back[block].astype(jnp.float32),
                False,
            )

        update_across(
            (their_gate, their_up), (got_gate.at[0], got_up.at[0]), their_step, lambda at: None
        )

    def average(mine, theirs):
        return (0.5 * (mine.astype(jnp.float32) + theirs.astype(jnp.float32))).astype(jnp.bfloat16)

    @pl.loop(0, n_chunks)
    def _(c):
        units = units_of(c)

        across_travels(c, lambda: sent(0, c).wait_recv())
        mixed_gate[:, units] = average(own_gate[c], got_gate[c])
        across_travels(c, lambda: sent(1, c).wait_recv())
        mixed_up[:, units] = average(own_up[c], got_up[c])
        sent(2, c).wait_recv()
        mixed_down[units] = average(own_down[c], got_down[c])

    @pl.loop(0, n_chunks)
    def _(c):
        across_travels(c, lambda: sent(0, c).wait_send())
        across_travels(c, lambda: sent(1, c).wait_send())
        sent(2, c).wait_send()

    for kind, h in both:
        for copy in (to_far, to_near, relay):
            copy(kind, h).wait_send()
    if early:
        for copy in weight_copies + [scalar_copy]:
            copy.wait_send()
        for h in range(2):
            to_peer(h).wait_send()
            for copy in (their_far, their_near, their_relay):
                copy(0, h).wait_send()

        @pl.loop(0, n_blocks)
        def _(block):
            back_copy(block).wait_send()


def one_level(level, early, count, round_index, rate, x, g, w_gate, w_up, w_down):
    seq, width = x.shape
    units = w_gate.shape[1]
    n_chunks, rows = units // CHUNK, 4 * seq
    bf16 = jnp.bfloat16
    hbm = pl.BlockSpec(memory_space=pltpu.HBM)
    vmem = pl.BlockSpec(memory_space=pltpu.VMEM)
    dma = pltpu.SemaphoreType.DMA
    across = pltpu.VMEM((n_chunks, width, CHUNK), bf16)
    along = pltpu.VMEM((n_chunks, CHUNK, width), bf16)
    raw = pltpu.VMEM((2, rows // BLOCK, BLOCK, width), bf16)
    column = pltpu.VMEM((width, CHUNK), bf16)
    backs = pltpu.VMEM((rows // BLOCK, BLOCK, CHUNK), bf16)
    scalar = pltpu.VMEM((8, 128), jnp.float32)
    partner = [pltpu.VMEM((1, rows // BLOCK, BLOCK, width), bf16)]
    partner += [column, column, backs, backs, scalar, scalar]
    partner += [dma((2,))] * 2 + [dma((1, 2))] * 6 + [dma((2,))] * 2
    partner += [dma((rows // BLOCK,))] * 2 + [dma((1,))] * 2
    mixed = pl.pallas_call(
        functools.partial(round_kernel, level, early),
        out_shape=[pltpu.VMEM(w.shape, bf16) for w in (w_gate, w_up, w_down)],
        in_specs=[hbm] * 8,
        out_specs=[vmem] * 3,
        scratch_shapes=[
            raw,
            pltpu.VMEM((rows, width), bf16),
            pltpu.VMEM((width, rows), bf16),
            pltpu.VMEM((rows, width), bf16),
            pltpu.VMEM(w_gate.shape, bf16),
            pltpu.VMEM(w_up.shape, bf16),
            pltpu.VMEM(w_down.shape, bf16),
            pltpu.VMEM((rows, 2 * CHUNK), bf16),
            pltpu.VMEM((rows, CHUNK), bf16),
            across,
            across,
            along,
            across,
            across,
            along,
            pltpu.SMEM((1,), jnp.int32),
            pltpu.SMEM((1,), jnp.int32),
            pltpu.SMEM((1,), jnp.float32),
            dma((10,)),
            dma((2, 2)),
            dma((2, 2)),
            dma((2, 2)),
            dma((2, 2)),
            dma((2, 2)),
            dma((2, 2)),
            dma((3, n_chunks)),
            dma((3, n_chunks)),
            *(partner if early else ()),
        ],
        compiler_params=pltpu.CompilerParams(
            collective_id=level, has_side_effects=True, vmem_limit_bytes=44 << 20
        ),
        cost_estimate=pl.CostEstimate(
            flops=12 * rows * width * units,
            bytes_accessed=2 * (6 * width * units + 2 * seq * width),
            transcendentals=rows * units,
        ),
        name=f"round_level_{level}",
    )(count, round_index, rate, x, g, w_gate, w_up, w_down)
    return write_out(*mixed)


def write_kernel(gate, up, down, out_gate, out_up, out_down, sem):
    copies = [
        pltpu.make_async_copy(src, dst, sem.at[i])
        for i, (src, dst) in enumerate(((gate, out_gate), (up, out_up), (down, out_down)))
    ]
    for copy in copies:
        copy.start()
    for copy in copies:
        copy.wait()


def write_out(*arrays):
    return pl.pallas_call(
        write_kernel,
        out_shape=[jax.ShapeDtypeStruct(a.shape, a.dtype) for a in arrays],
        in_specs=[pl.BlockSpec(memory_space=pltpu.VMEM)] * 3,
        out_specs=[pl.BlockSpec(memory_space=pltpu.HBM)] * 3,
        scratch_shapes=[pltpu.SemaphoreType.DMA((3,))],
        compiler_params=pltpu.CompilerParams(vmem_limit_bytes=16 << 20),
        name="write_out",
    )(*arrays)


def per_device(inputs, upstream, counts, round_index, rates, gate_weight, up_weight, down_weight):
    levels = lax.axis_size("node").bit_length() - 1
    mixed = lax.switch(
        lax.rem(round_index[0], levels),
        [functools.partial(one_level, level, level < levels - 1) for level in range(levels)],
        counts,
        round_index,
        rates,
        inputs[0],
        upstream[0],
        gate_weight[0],
        up_weight[0],
        down_weight[0],
    )
    return tuple(m[None] for m in mixed)


def solution(mesh):
    return jax.shard_map(
        per_device,
        mesh=mesh,
        in_specs=(
            P("node", "shard", None),
            P("node", "shard", None),
            P("node"),
            P(),
            P("node"),
            P("node", None, "shard"),
            P("node", None, "shard"),
            P("node", "shard", None),
        ),
        out_specs=(P("node", None, "shard"), P("node", None, "shard"), P("node", "shard", None)),
        check_vma=False,
    )
```

```python
import functools

import jax
import jax.numpy as jnp
from jax import lax
from jax.experimental import pallas as pl
from jax.experimental.pallas import tpu as pltpu
from jax.sharding import PartitionSpec as P

MESH = pl.DeviceIdType.MESH
CHUNK = 128
BLOCK = 128
PIECE = 64
PARTS = 3

EARLY = ((0, 0, 5), (1, 0, 6), (0, 1, 7))
FIRST_LATE = min(blocks for _, _, blocks in EARLY)


def remote(src, dst, send_sem, recv_sem, device):
    return pltpu.make_async_remote_copy(
        src_ref=src,
        dst_ref=dst,
        send_sem=send_sem,
        recv_sem=recv_sem,
        device_id=device,
        device_id_type=MESH,
    )


def round_kernel(
    level,
    early,
    count_hbm,
    round_hbm,
    rate_hbm,
    x_hbm,
    g_hbm,
    wg_hbm,
    wu_hbm,
    wd_hbm,
    mixed_gate,
    mixed_up,
    mixed_down,
    raw,
    normed,
    normed_t,
    grad_out,
    w_gate,
    w_up,
    w_down,
    d_both,
    hidden,
    own_gate,
    own_up,
    own_down,
    got_gate,
    got_up,
    got_down,
    count_ref,
    round_ref,
    rate_ref,
    local_sem,
    near_send,
    near_recv,
    far_send,
    far_recv,
    relay_send,
    relay_recv,
    chunk_send,
    chunk_recv,
    *partner,
):
    node, shard = lax.axis_index("node"), lax.axis_index("shard")
    core, chip = lax.rem(shard, 2), shard // 2
    near = (node, chip * 2 + 1 - core)
    far = (node, (1 - chip) * 2 + core)
    stride = 1 << level
    peer = (node + (1 - 2 * lax.rem(node // stride, 2)) * stride, shard)
    n_blocks = raw.shape[1]
    width = normed.shape[1]
    n_chunks = own_gate.shape[0]

    def load(i, src, dst):
        return pltpu.make_async_copy(src, dst, local_sem.at[i])

    def rows_of(h):
        return pl.ds(h * BLOCK, BLOCK)

    slot_loads = [
        load(kind * 2 + h, src.at[rows_of(h)], raw.at[kind, h])
        for h in range(2)
        for kind, src in enumerate((x_hbm, g_hbm))
    ]
    other_loads = [
        load(4, wg_hbm, w_gate),
        load(5, wu_hbm, w_up),
        load(6, wd_hbm, w_down),
        load(7, count_hbm, count_ref),
        load(8, round_hbm, round_ref),
        load(9, rate_hbm, rate_ref),
    ]
    for copy in slot_loads:
        copy.start()

    barrier = pltpu.get_barrier_semaphore()
    for device in (near, far, peer):
        pl.semaphore_signal(barrier, inc=1, device_id=device, device_id_type=MESH)
    pl.semaphore_wait(barrier, 3)

    n_pieces = n_blocks - 4
    per_block = BLOCK // PIECE
    head, tail = pl.ds(0, PIECE), pl.ds(PIECE, PIECE)

    def own_piece(kind, i):
        start = pl.multiple_of((i % per_block) * PIECE, PIECE)
        return raw.at[kind, i // per_block, pl.ds(start, PIECE)]

    def to_near(kind, h):
        return remote(
            raw.at[kind, h], raw.at[kind, 2 + h], near_send.at[kind, h], near_recv.at[kind, h], near
        )

    def to_far(kind, i):
        return remote(
            own_piece(kind, i),
            raw.at[kind, 4 + i, head],
            far_send.at[kind, i],
            far_recv.at[kind, i],
            far,
        )

    def relay(kind, i):
        return remote(
            raw.at[kind, 4 + i, head],
            raw.at[kind, 4 + i, tail],
            relay_send.at[kind, i],
            relay_recv.at[kind, i],
            near,
        )

    both = [(kind, h) for h in range(2) for kind in range(2)]
    pieces = [(kind, i) for i in range(n_pieces) for kind in range(2)]
    pairs = ((own_gate, got_gate), (own_up, got_up), (own_down, got_down))
    if early:
        (passing, theirs, partial, late, their_late, scalars, their_scalars, *sems) = partner
        slot_sems, far_sems, relay_sems, late_sems, scalar_sems = (
            sems[i : i + 2] for i in range(0, 10, 2)
        )
        skipped = FIRST_LATE - 4
        late_blocks = range(skipped, n_pieces)

        def to_peer(j):
            return remote(
                own_piece(0, j + skipped),
                passing.at[j],
                slot_sems[0].at[j],
                slot_sems[1].at[j],
                peer,
            )

        def their_far(j):
            return remote(
                passing.at[j], theirs.at[0, j, head], far_sems[0].at[j], far_sems[1].at[j], far
            )

        def their_relay(j):
            return remote(
                theirs.at[0, j, head],
                theirs.at[0, j, tail],
                relay_sems[0].at[j],
                relay_sems[1].at[j],
                near,
            )

        def late_copy(item, j):
            rows = pl.ds(pl.multiple_of(j * BLOCK, BLOCK), BLOCK)
            return remote(
                late.at[item, rows],
                their_late.at[item, rows],
                late_sems[0].at[item, j],
                late_sems[1].at[item, j],
                peer,
            )

        def early_copy(item, at=None):
            k, c, _ = EARLY[item]
            mine, other = partial.at[item], pairs[k][1].at[c]
            if at is not None:
                mine, other = mine.at[at], other.at[at]
            return remote(mine, other, chunk_send.at[k, c], chunk_recv.at[k, c], peer)

        scalar_copy = remote(
            scalars, their_scalars, scalar_sems[0].at[0], scalar_sems[1].at[0], peer
        )

    for h in range(2):
        for kind in range(2):
            slot_loads[2 * h + kind].wait()
        for i in range(h * per_block, (h + 1) * per_block):
            for kind in range(2):
                to_far(kind, i).start()
            if early and i >= skipped:
                to_peer(i - skipped).start()
    for copy in other_loads:
        copy.start()
    for kind, h in both:
        to_near(kind, h).start()
    for copy in other_loads:
        copy.wait()

    decay = 250.0 / (250.0 + jnp.full((8, 128), round_ref[0], jnp.int32).astype(jnp.float32))
    step = jnp.max(rate_ref[0] * decay)
    count = count_ref[0].astype(jnp.float32)
    if early:
        scalars[...] = rate_ref[0] * decay

    def prepare(blocks, block, count):
        to = pl.ds(pl.multiple_of(block * BLOCK, BLOCK), BLOCK)
        floats = blocks[0, block].astype(jnp.float32)
        scale = lax.rsqrt(jnp.mean(floats * floats, -1, keepdims=True) + 1e-06)
        value = (floats * scale).astype(jnp.bfloat16)
        normed[to] = value
        normed_t[:, to] = value.T
        if count is None:
            return
        for half, rest in ((0, 2), (1, 3)):
            slot = lax.bitwise_xor(shard, jnp.where(block < 4, block // 2, rest))
            live = jnp.where(slot.astype(jnp.float32) < count, 1.0, 0.0)
            start = pl.multiple_of(block * BLOCK + half * PIECE, PIECE)
            grad_out[pl.ds(start, PIECE)] = (
                blocks[1, block, half * PIECE : (half + 1) * PIECE].astype(jnp.float32) * live
            ).astype(jnp.bfloat16)

    def units_of(c):
        return pl.ds(pl.multiple_of(c * CHUNK, CHUNK), CHUNK)

    def own_weights(c):
        units = units_of(c)
        return w_gate.at[:, units], w_up.at[:, units], w_down.at[units]

    def forward(c, block):
        gate_weight, up_weight, down_weight = own_weights(c)
        buffer = lax.rem(c, 2)
        at = pl.ds(pl.multiple_of(block * BLOCK, BLOCK), BLOCK)
        n = normed[at]
        gate = jnp.dot(n, gate_weight[...], preferred_element_type=jnp.float32)
        up = jnp.dot(n, up_weight[...], preferred_element_type=jnp.float32)
        back = lax.dot_general(
            grad_out[at],
            down_weight[...],
            (((1,), (1,)), ((), ())),
            preferred_element_type=jnp.float32,
        )
        k = 0.7978845608028654
        square = gate * gate
        t = jnp.tanh(gate * (k + (k * 0.044715) * square))
        half = 0.5 + 0.5 * t
        act = gate * half
        slope = half + (0.5 * gate) * (1.0 - t * t) * (k + (3.0 * k * 0.044715) * square)
        hidden[buffer, at] = (act * up).astype(jnp.bfloat16)
        d_both[buffer, at, :CHUNK] = (back * up * slope).astype(jnp.bfloat16)
        d_both[buffer, at, CHUNK:] = (back * act).astype(jnp.bfloat16)

    part = width // PARTS

    def part_of(b):
        return pl.ds(pl.multiple_of(b * part, part), part)

    def send_early(item):
        k, c, blocks = EARLY[item]
        weight = own_weights(c)[k]
        rows = blocks * BLOCK

        @pl.loop(0, PARTS)
        def _(b):
            at = part_of(b)
            grad = jnp.dot(
                normed_t[at, :rows],
                d_both[c, :rows, k * CHUNK : (k + 1) * CHUNK],
                preferred_element_type=jnp.float32,
            )
            partial[item, at] = (weight[at].astype(jnp.float32) - step * grad).astype(
                jnp.bfloat16
            )
            early_copy(item, at).start()

    def send_late(item, block):
        k, c, _ = EARLY[item]
        at = pl.ds(pl.multiple_of(block * BLOCK, BLOCK), BLOCK)
        to = pl.ds(pl.multiple_of((block - FIRST_LATE) * BLOCK, BLOCK), BLOCK)
        late[item, to] = d_both[c, at, k * CHUNK : (k + 1) * CHUNK]
        late_copy(item, block - FIRST_LATE).start()

    ahead = 2 if early else 1

    @pl.loop(0, n_blocks)
    def _(block):
        @pl.when(block == 2)
        def _():
            for kind, h in both:
                to_near(kind, h).wait_recv()

        @pl.when(block >= 4)
        def _():
            for kind in range(2):
                to_far(kind, block - 4).wait_recv()
                relay(kind, block - 4).start()
            for kind in range(2):
                relay(kind, block - 4).wait_recv()

        prepare(raw, block, count)
        for c in range(ahead):
            forward(c, block)
        if early:
            for item, (_, _, blocks) in enumerate(EARLY):
                pl.when(block >= blocks)(functools.partial(send_late, item, block))
            for item, (_, _, blocks) in enumerate(EARLY):
                pl.when(block == blocks - 1)(functools.partial(send_early, item))

    if early:
        scalar_copy.start()
        for j in range(len(late_blocks)):
            to_peer(j).wait_recv()
            their_far(j).start()

    def sent(k, c, at=None):
        mine, other = (ref.at[c] if at is None else ref.at[c, at] for ref in pairs[k])
        return remote(mine, other, chunk_send.at[k, c], chunk_recv.at[k, c], peer)

    def if_late(k, c, act):
        chunks = [chunk for matrix, chunk, _ in EARLY if matrix == k] if early else []
        if chunks:
            pl.when(c > max(chunks))(act)
        else:
            act()

    @pl.loop(0, n_chunks)
    def _(c):
        gate_weight, up_weight, down_weight = own_weights(c)
        buffer = lax.rem(c, 2)

        hidden_t = hidden[buffer].T

        @pl.loop(0, PARTS)
        def _(b):
            at = part_of(b)
            grad = jnp.dot(normed_t[at], d_both[buffer], preferred_element_type=jnp.float32)
            own_gate[c, at] = (
                gate_weight[at].astype(jnp.float32) - step * grad[:, :CHUNK]
            ).astype(jnp.bfloat16)
            own_up[c, at] = (
                up_weight[at].astype(jnp.float32) - step * grad[:, CHUNK:]
            ).astype(jnp.bfloat16)
            for k in range(2):
                if_late(k, c, lambda: sent(k, c, at).start())

        @pl.loop(0, PARTS)
        def _(b):
            at = part_of(b)
            grad = jnp.dot(hidden_t, grad_out[:, at], preferred_element_type=jnp.float32)
            own_down[c, :, at] = (
                down_weight[:, at].astype(jnp.float32) - step * grad
            ).astype(jnp.bfloat16)

        sent(2, c).start()

        @pl.when(c < n_chunks - ahead)
        def _():
            @pl.loop(0, n_blocks)
            def _(block):
                forward(c + ahead, block)

    if early:
        for j in range(len(late_blocks)):
            their_far(j).wait_recv()
            their_relay(j).start()
        for item, (_, _, blocks) in enumerate(EARLY):
            early_copy(item).wait_recv()
            for j in range(len(late_blocks)):
                if FIRST_LATE + j >= blocks:
                    late_copy(item, j).wait_recv()
                else:
                    their_late[item, j * BLOCK : (j + 1) * BLOCK] = jnp.zeros(
                        (BLOCK, CHUNK), jnp.bfloat16
                    )
        scalar_copy.wait_recv()
        for j in range(len(late_blocks)):
            their_relay(j).wait_recv()
        their_step = jnp.max(their_scalars[...])

        @pl.loop(0, len(late_blocks))
        def _(j):
            prepare(theirs, j, None)

        for item, (k, c, _) in enumerate(EARLY):
            result = pairs[k][1].at[c]

            @pl.loop(0, PARTS)
            def _(b):
                at = part_of(b)
                grad = jnp.dot(
                    normed_t[at, : len(late_blocks) * BLOCK],
                    their_late[item],
                    preferred_element_type=jnp.float32,
                )
                result[at] = (result[at].astype(jnp.float32) - their_step * grad).astype(
                    jnp.bfloat16
                )

    def average(mine, theirs):
        return (0.5 * (mine.astype(jnp.float32) + theirs.astype(jnp.float32))).astype(jnp.bfloat16)

    @pl.loop(0, n_chunks)
    def _(c):
        units = units_of(c)

        if_late(0, c, lambda: sent(0, c).wait_recv())
        mixed_gate[:, units] = average(own_gate[c], got_gate[c])
        if_late(1, c, lambda: sent(1, c).wait_recv())
        mixed_up[:, units] = average(own_up[c], got_up[c])
        sent(2, c).wait_recv()
        mixed_down[units] = average(own_down[c], got_down[c])

    @pl.loop(0, n_chunks)
    def _(c):
        if_late(0, c, lambda: sent(0, c).wait_send())
        if_late(1, c, lambda: sent(1, c).wait_send())
        sent(2, c).wait_send()

    for kind, h in both:
        to_near(kind, h).wait_send()
    for kind, i in pieces:
        to_far(kind, i).wait_send()
        relay(kind, i).wait_send()
    if early:
        scalar_copy.wait_send()
        for j in range(len(late_blocks)):
            to_peer(j).wait_send()
            their_far(j).wait_send()
            their_relay(j).wait_send()
        for item, (_, _, blocks) in enumerate(EARLY):
            early_copy(item).wait_send()
            for j in range(blocks - FIRST_LATE, len(late_blocks)):
                late_copy(item, j).wait_send()


def one_level(level, early, count, round_index, rate, x, g, w_gate, w_up, w_down):
    seq, width = x.shape
    units = w_gate.shape[1]
    n_chunks, rows = units // CHUNK, 4 * seq
    bf16 = jnp.bfloat16
    hbm = pl.BlockSpec(memory_space=pltpu.HBM)
    vmem = pl.BlockSpec(memory_space=pltpu.VMEM)
    dma = pltpu.SemaphoreType.DMA
    across = pltpu.VMEM((n_chunks, width, CHUNK), bf16)
    along = pltpu.VMEM((n_chunks, CHUNK, width), bf16)
    raw = pltpu.VMEM((2, rows // BLOCK, BLOCK, width), bf16)
    n_pieces = seq // PIECE
    n_late = 4 + n_pieces - FIRST_LATE
    late = pltpu.VMEM((len(EARLY), n_late * BLOCK, CHUNK), bf16)
    scalar = pltpu.VMEM((8, 128), jnp.float32)
    partner = [
        pltpu.VMEM((n_late, PIECE, width), bf16),
        pltpu.VMEM((1, n_late, BLOCK, width), bf16),
        pltpu.VMEM((len(EARLY), width, CHUNK), bf16),
        late,
        late,
        scalar,
        scalar,
    ]
    partner += [dma((n_late,))] * 6 + [dma((len(EARLY), n_late))] * 2 + [dma((1,))] * 2
    mixed = pl.pallas_call(
        functools.partial(round_kernel, level, early),
        out_shape=[pltpu.VMEM(w.shape, bf16) for w in (w_gate, w_up, w_down)],
        in_specs=[hbm] * 8,
        out_specs=[vmem] * 3,
        scratch_shapes=[
            raw,
            pltpu.VMEM((rows, width), bf16),
            pltpu.VMEM((width, rows), bf16),
            pltpu.VMEM((rows, width), bf16),
            pltpu.VMEM(w_gate.shape, bf16),
            pltpu.VMEM(w_up.shape, bf16),
            pltpu.VMEM(w_down.shape, bf16),
            pltpu.VMEM((2, rows, 2 * CHUNK), bf16),
            pltpu.VMEM((2, rows, CHUNK), bf16),
            across,
            across,
            along,
            across,
            across,
            along,
            pltpu.SMEM((1,), jnp.int32),
            pltpu.SMEM((1,), jnp.int32),
            pltpu.SMEM((1,), jnp.float32),
            dma((10,)),
            dma((2, 2)),
            dma((2, 2)),
            dma((2, n_pieces)),
            dma((2, n_pieces)),
            dma((2, n_pieces)),
            dma((2, n_pieces)),
            dma((3, n_chunks)),
            dma((3, n_chunks)),
            *(partner if early else ()),
        ],
        compiler_params=pltpu.CompilerParams(
            collective_id=level, has_side_effects=True, vmem_limit_bytes=44 << 20
        ),
        cost_estimate=pl.CostEstimate(
            flops=12 * rows * width * units,
            bytes_accessed=2 * (6 * width * units + 2 * seq * width),
            transcendentals=rows * units,
        ),
        name=f"round_level_{level}",
    )(count, round_index, rate, x, g, w_gate, w_up, w_down)
    return write_out(*mixed)


def write_kernel(gate, up, down, out_gate, out_up, out_down, sem):
    copies = [
        pltpu.make_async_copy(src, dst, sem.at[i])
        for i, (src, dst) in enumerate(((gate, out_gate), (up, out_up), (down, out_down)))
    ]
    for copy in copies:
        copy.start()
    for copy in copies:
        copy.wait()


def write_out(*arrays):
    return pl.pallas_call(
        write_kernel,
        out_shape=[jax.ShapeDtypeStruct(a.shape, a.dtype) for a in arrays],
        in_specs=[pl.BlockSpec(memory_space=pltpu.VMEM)] * 3,
        out_specs=[pl.BlockSpec(memory_space=pltpu.HBM)] * 3,
        scratch_shapes=[pltpu.SemaphoreType.DMA((3,))],
        compiler_params=pltpu.CompilerParams(vmem_limit_bytes=16 << 20),
        name="write_out",
    )(*arrays)


def per_device(inputs, upstream, counts, round_index, rates, gate_weight, up_weight, down_weight):
    levels = lax.axis_size("node").bit_length() - 1
    mixed = lax.switch(
        lax.rem(round_index[0], levels),
        [functools.partial(one_level, level, level < levels - 1) for level in range(levels)],
        counts,
        round_index,
        rates,
        inputs[0],
        upstream[0],
        gate_weight[0],
        up_weight[0],
        down_weight[0],
    )
    return tuple(m[None] for m in mixed)


def solution(mesh):
    return jax.shard_map(
        per_device,
        mesh=mesh,
        in_specs=(
            P("node", "shard", None),
            P("node", "shard", None),
            P("node"),
            P(),
            P("node"),
            P("node", None, "shard"),
            P("node", None, "shard"),
            P("node", "shard", None),
        ),
        out_specs=(P("node", None, "shard"), P("node", None, "shard"), P("node", "shard", None)),
        check_vma=False,
    )
```

```python
import functools

import jax
import jax.numpy as jnp
from jax import lax
from jax.experimental import pallas as pl
from jax.experimental.pallas import tpu as pltpu
from jax.sharding import PartitionSpec as P

MESH = pl.DeviceIdType.MESH
CHUNK = 128
BLOCK = 128
PIECE = 64
PARTS = 3

EARLY = ((0, 0, 5), (1, 0, 6), (0, 1, 7))
EARLY_SHARED = ((0, 0, 7),)


def first_late(early):
    return min(blocks for _, _, blocks in early)


def remote(src, dst, send_sem, recv_sem, device):
    return pltpu.make_async_remote_copy(
        src_ref=src,
        dst_ref=dst,
        send_sem=send_sem,
        recv_sem=recv_sem,
        device_id=device,
        device_id_type=MESH,
    )


def round_kernel(
    level,
    early,
    direct,
    count_hbm,
    round_hbm,
    rate_hbm,
    x_hbm,
    g_hbm,
    wg_hbm,
    wu_hbm,
    wd_hbm,
    mixed_gate,
    mixed_up,
    mixed_down,
    raw,
    normed,
    normed_t,
    grad_out,
    w_gate,
    w_up,
    w_down,
    d_both,
    hidden,
    own_gate,
    own_up,
    own_down,
    got_gate,
    got_up,
    got_down,
    count_ref,
    round_ref,
    rate_ref,
    local_sem,
    near_send,
    near_recv,
    far_send,
    far_recv,
    relay_send,
    relay_recv,
    chunk_send,
    chunk_recv,
    passing,
    theirs,
    partial,
    late,
    their_late,
    scalars,
    their_scalars,
    slot_send,
    slot_recv,
    across_send,
    across_recv,
    pass_send,
    pass_recv,
    late_send,
    late_recv,
    scalar_send,
    scalar_recv,
):
    node, shard = lax.axis_index("node"), lax.axis_index("shard")
    core, chip = lax.rem(shard, 2), shard // 2
    near = (node, chip * 2 + 1 - core)
    far = (node, (1 - chip) * 2 + core)
    stride = 1 << level
    other = node + (1 - 2 * lax.rem(node // stride, 2)) * stride
    peer, cross = (other, shard), (other, far[1])
    n_blocks = raw.shape[1]
    width = normed.shape[1]
    n_chunks = own_gate.shape[0]

    def load(i, src, dst):
        return pltpu.make_async_copy(src, dst, local_sem.at[i])

    def rows_of(h):
        return pl.ds(h * BLOCK, BLOCK)

    slot_loads = [
        load(kind * 2 + h, src.at[rows_of(h)], raw.at[kind, h])
        for h in range(2)
        for kind, src in enumerate((x_hbm, g_hbm))
    ]
    other_loads = [
        load(4, wg_hbm, w_gate),
        load(5, wu_hbm, w_up),
        load(6, wd_hbm, w_down),
        load(7, count_hbm, count_ref),
        load(8, round_hbm, round_ref),
        load(9, rate_hbm, rate_ref),
    ]
    for copy in slot_loads:
        copy.start()

    barrier = pltpu.get_barrier_semaphore()
    group = (near, far, peer, cross) if direct else (near, far, peer)
    for device in group:
        pl.semaphore_signal(barrier, inc=1, device_id=device, device_id_type=MESH)
    pl.semaphore_wait(barrier, len(group))

    n_pieces = n_blocks - 4
    per_block = BLOCK // PIECE
    head, tail = pl.ds(0, PIECE), pl.ds(PIECE, PIECE)

    def own_piece(kind, i):
        start = pl.multiple_of((i % per_block) * PIECE, PIECE)
        return raw.at[kind, i // per_block, pl.ds(start, PIECE)]

    def to_near(kind, h):
        return remote(
            raw.at[kind, h], raw.at[kind, 2 + h], near_send.at[kind, h], near_recv.at[kind, h], near
        )

    def to_far(kind, i):
        return remote(
            own_piece(kind, i),
            raw.at[kind, 4 + i, head],
            far_send.at[kind, i],
            far_recv.at[kind, i],
            far,
        )

    def relay(kind, i):
        return remote(
            raw.at[kind, 4 + i, head],
            raw.at[kind, 4 + i, tail],
            relay_send.at[kind, i],
            relay_recv.at[kind, i],
            near,
        )

    both = [(kind, h) for h in range(2) for kind in range(2)]
    pieces = [(kind, i) for i in range(n_pieces) for kind in range(2)]
    pairs = ((own_gate, got_gate), (own_up, got_up), (own_down, got_down))
    first = first_late(early)
    skipped = first - 4
    n_late = n_pieces - skipped

    def to_other(j):
        return remote(
            own_piece(0, j + skipped),
            theirs.at[0, j, head] if direct else passing.at[j],
            slot_send.at[j],
            slot_recv.at[j],
            cross if direct else peer,
        )

    def across(j):
        return remote(
            passing.at[j], theirs.at[0, j, head], across_send.at[j], across_recv.at[j], far
        )

    def pass_on(j):
        return remote(
            theirs.at[0, j, head], theirs.at[0, j, tail], pass_send.at[j], pass_recv.at[j], near
        )

    def late_copy(item, j):
        rows = pl.ds(pl.multiple_of(j * BLOCK, BLOCK), BLOCK)
        return remote(
            late.at[item, rows],
            their_late.at[item, rows],
            late_send.at[item, j],
            late_recv.at[item, j],
            peer,
        )

    def early_copy(item, at=None):
        k, c, _ = early[item]
        mine, got = partial.at[item], pairs[k][1].at[c]
        if at is not None:
            mine, got = mine.at[at], got.at[at]
        return remote(mine, got, chunk_send.at[k, c], chunk_recv.at[k, c], peer)

    scalar_copy = remote(scalars, their_scalars, scalar_send.at[0], scalar_recv.at[0], peer)

    for h in range(2):
        for kind in range(2):
            slot_loads[2 * h + kind].wait()
        for i in range(h * per_block, (h + 1) * per_block):
            for kind in range(2):
                to_far(kind, i).start()
            if i >= skipped:
                to_other(i - skipped).start()
    for copy in other_loads:
        copy.start()
    for kind, h in both:
        to_near(kind, h).start()
    for copy in other_loads:
        copy.wait()

    decay = 250.0 / (250.0 + jnp.full((8, 128), round_ref[0], jnp.int32).astype(jnp.float32))
    step = jnp.max(rate_ref[0] * decay)
    count = count_ref[0].astype(jnp.float32)
    scalars[...] = rate_ref[0] * decay

    def prepare(blocks, block, count):
        to = pl.ds(pl.multiple_of(block * BLOCK, BLOCK), BLOCK)
        floats = blocks[0, block].astype(jnp.float32)
        scale = lax.rsqrt(jnp.mean(floats * floats, -1, keepdims=True) + 1e-06)
        value = (floats * scale).astype(jnp.bfloat16)
        normed[to] = value
        normed_t[:, to] = value.T
        if count is None:
            return
        for half, rest in ((0, 2), (1, 3)):
            slot = lax.bitwise_xor(shard, jnp.where(block < 4, block // 2, rest))
            live = jnp.where(slot.astype(jnp.float32) < count, 1.0, 0.0)
            start = pl.multiple_of(block * BLOCK + half * PIECE, PIECE)
            grad_out[pl.ds(start, PIECE)] = (
                blocks[1, block, half * PIECE : (half + 1) * PIECE].astype(jnp.float32) * live
            ).astype(jnp.bfloat16)

    def units_of(c):
        return pl.ds(pl.multiple_of(c * CHUNK, CHUNK), CHUNK)

    def own_weights(c):
        units = units_of(c)
        return w_gate.at[:, units], w_up.at[:, units], w_down.at[units]

    def forward(c, block):
        gate_weight, up_weight, down_weight = own_weights(c)
        buffer = lax.rem(c, 2)
        at = pl.ds(pl.multiple_of(block * BLOCK, BLOCK), BLOCK)
        n = normed[at]
        gate = jnp.dot(n, gate_weight[...], preferred_element_type=jnp.float32)
        up = jnp.dot(n, up_weight[...], preferred_element_type=jnp.float32)
        back = lax.dot_general(
            grad_out[at],
            down_weight[...],
            (((1,), (1,)), ((), ())),
            preferred_element_type=jnp.float32,
        )
        k = 0.7978845608028654
        square = gate * gate
        t = jnp.tanh(gate * (k + (k * 0.044715) * square))
        half = 0.5 + 0.5 * t
        act = gate * half
        slope = half + (0.5 * gate) * (1.0 - t * t) * (k + (3.0 * k * 0.044715) * square)
        hidden[buffer, at] = (act * up).astype(jnp.bfloat16)
        d_both[buffer, at, :CHUNK] = (back * up * slope).astype(jnp.bfloat16)
        d_both[buffer, at, CHUNK:] = (back * act).astype(jnp.bfloat16)

    part = width // PARTS

    def part_of(b):
        return pl.ds(pl.multiple_of(b * part, part), part)

    def send_early(item):
        k, c, blocks = early[item]
        weight = own_weights(c)[k]
        rows = blocks * BLOCK

        @pl.loop(0, PARTS)
        def _(b):
            at = part_of(b)
            grad = jnp.dot(
                normed_t[at, :rows],
                d_both[c, :rows, k * CHUNK : (k + 1) * CHUNK],
                preferred_element_type=jnp.float32,
            )
            partial[item, at] = (weight[at].astype(jnp.float32) - step * grad).astype(
                jnp.bfloat16
            )
            early_copy(item, at).start()

    def send_late(item, block):
        k, c, _ = early[item]
        at = pl.ds(pl.multiple_of(block * BLOCK, BLOCK), BLOCK)
        to = pl.ds(pl.multiple_of((block - first) * BLOCK, BLOCK), BLOCK)
        late[item, to] = d_both[c, at, k * CHUNK : (k + 1) * CHUNK]
        late_copy(item, block - first).start()

    ahead = 1 + max(c for _, c, _ in early)

    @pl.loop(0, n_blocks)
    def _(block):
        @pl.when(block == 2)
        def _():
            for kind, h in both:
                to_near(kind, h).wait_recv()

        @pl.when(block >= 4)
        def _():
            for kind in range(2):
                to_far(kind, block - 4).wait_recv()
                relay(kind, block - 4).start()
            for kind in range(2):
                relay(kind, block - 4).wait_recv()

        prepare(raw, block, count)
        for c in range(ahead):
            forward(c, block)
            items = [(item, blocks) for item, (_, chunk, blocks) in enumerate(early) if chunk == c]
            for item, blocks in items:
                pl.when(block >= blocks)(functools.partial(send_late, item, block))
            for item, blocks in items:
                pl.when(block == blocks - 1)(functools.partial(send_early, item))

    scalar_copy.start()
    if not direct:
        for j in range(n_late):
            to_other(j).wait_recv()
            across(j).start()

    def sent(k, c, at=None):
        mine, other = (ref.at[c] if at is None else ref.at[c, at] for ref in pairs[k])
        return remote(mine, other, chunk_send.at[k, c], chunk_recv.at[k, c], peer)

    def if_late(k, c, act):
        chunks = [chunk for matrix, chunk, _ in early if matrix == k]
        if chunks:
            pl.when(c > max(chunks))(act)
        else:
            act()

    @pl.loop(0, n_chunks)
    def _(c):
        gate_weight, up_weight, down_weight = own_weights(c)
        buffer = lax.rem(c, 2)

        hidden_t = hidden[buffer].T

        @pl.loop(0, PARTS)
        def _(b):
            at = part_of(b)
            grad = jnp.dot(normed_t[at], d_both[buffer], preferred_element_type=jnp.float32)
            own_gate[c, at] = (
                gate_weight[at].astype(jnp.float32) - step * grad[:, :CHUNK]
            ).astype(jnp.bfloat16)
            own_up[c, at] = (
                up_weight[at].astype(jnp.float32) - step * grad[:, CHUNK:]
            ).astype(jnp.bfloat16)
            for k in range(2):
                if_late(k, c, lambda: sent(k, c, at).start())

        @pl.loop(0, PARTS)
        def _(b):
            at = part_of(b)
            grad = jnp.dot(hidden_t, grad_out[:, at], preferred_element_type=jnp.float32)
            own_down[c, :, at] = (
                down_weight[:, at].astype(jnp.float32) - step * grad
            ).astype(jnp.bfloat16)

        sent(2, c).start()

        @pl.when(c < n_chunks - ahead)
        def _():
            @pl.loop(0, n_blocks)
            def _(block):
                forward(c + ahead, block)

    for j in range(n_late):
        (to_other if direct else across)(j).wait_recv()
        pass_on(j).start()
    for item, (_, _, blocks) in enumerate(early):
        early_copy(item).wait_recv()
        for j in range(n_late):
            if first + j >= blocks:
                late_copy(item, j).wait_recv()
            else:
                their_late[item, j * BLOCK : (j + 1) * BLOCK] = jnp.zeros(
                    (BLOCK, CHUNK), jnp.bfloat16
                )
    scalar_copy.wait_recv()
    for j in range(n_late):
        pass_on(j).wait_recv()
    their_step = jnp.max(their_scalars[...])

    @pl.loop(0, n_late)
    def _(j):
        prepare(theirs, j, None)

    for item, (k, c, _) in enumerate(early):
        result = pairs[k][1].at[c]

        @pl.loop(0, PARTS)
        def _(b):
            at = part_of(b)
            grad = jnp.dot(
                normed_t[at, : n_late * BLOCK],
                their_late[item],
                preferred_element_type=jnp.float32,
            )
            result[at] = (result[at].astype(jnp.float32) - their_step * grad).astype(jnp.bfloat16)

    def average(mine, theirs):
        return (0.5 * (mine.astype(jnp.float32) + theirs.astype(jnp.float32))).astype(jnp.bfloat16)

    @pl.loop(0, n_chunks)
    def _(c):
        units = units_of(c)

        if_late(0, c, lambda: sent(0, c).wait_recv())
        mixed_gate[:, units] = average(own_gate[c], got_gate[c])
        if_late(1, c, lambda: sent(1, c).wait_recv())
        mixed_up[:, units] = average(own_up[c], got_up[c])
        sent(2, c).wait_recv()
        mixed_down[units] = average(own_down[c], got_down[c])

    @pl.loop(0, n_chunks)
    def _(c):
        if_late(0, c, lambda: sent(0, c).wait_send())
        if_late(1, c, lambda: sent(1, c).wait_send())
        sent(2, c).wait_send()

    for kind, h in both:
        to_near(kind, h).wait_send()
    for kind, i in pieces:
        to_far(kind, i).wait_send()
        relay(kind, i).wait_send()
    scalar_copy.wait_send()
    for j in range(n_late):
        to_other(j).wait_send()
        if not direct:
            across(j).wait_send()
        pass_on(j).wait_send()
    for item, (_, _, blocks) in enumerate(early):
        early_copy(item).wait_send()
        for j in range(blocks - first, n_late):
            late_copy(item, j).wait_send()


def one_level(level, shared, count, round_index, rate, x, g, w_gate, w_up, w_down):
    seq, width = x.shape
    units = w_gate.shape[1]
    n_chunks, rows = units // CHUNK, 4 * seq
    bf16 = jnp.bfloat16
    hbm = pl.BlockSpec(memory_space=pltpu.HBM)
    vmem = pl.BlockSpec(memory_space=pltpu.VMEM)
    dma = pltpu.SemaphoreType.DMA
    across = pltpu.VMEM((n_chunks, width, CHUNK), bf16)
    along = pltpu.VMEM((n_chunks, CHUNK, width), bf16)
    raw = pltpu.VMEM((2, rows // BLOCK, BLOCK, width), bf16)
    n_pieces = seq // PIECE
    early = EARLY_SHARED if shared else EARLY
    n_late = 4 + n_pieces - first_late(early)
    late = pltpu.VMEM((len(early), n_late * BLOCK, CHUNK), bf16)
    scalar = pltpu.VMEM((8, 128), jnp.float32)
    partner = [
        pltpu.VMEM((n_late, PIECE, width), bf16),
        pltpu.VMEM((1, n_late, BLOCK, width), bf16),
        pltpu.VMEM((len(early), width, CHUNK), bf16),
        late,
        late,
        scalar,
        scalar,
    ]
    partner += [dma((n_late,))] * 6 + [dma((len(early), n_late))] * 2 + [dma((1,))] * 2
    mixed = pl.pallas_call(
        functools.partial(round_kernel, level, early, shared),
        out_shape=[pltpu.VMEM(w.shape, bf16) for w in (w_gate, w_up, w_down)],
        in_specs=[hbm] * 8,
        out_specs=[vmem] * 3,
        scratch_shapes=[
            raw,
            pltpu.VMEM((rows, width), bf16),
            pltpu.VMEM((width, rows), bf16),
            pltpu.VMEM((rows, width), bf16),
            pltpu.VMEM(w_gate.shape, bf16),
            pltpu.VMEM(w_up.shape, bf16),
            pltpu.VMEM(w_down.shape, bf16),
            pltpu.VMEM((2, rows, 2 * CHUNK), bf16),
            pltpu.VMEM((2, rows, CHUNK), bf16),
            across,
            across,
            along,
            across,
            across,
            along,
            pltpu.SMEM((1,), jnp.int32),
            pltpu.SMEM((1,), jnp.int32),
            pltpu.SMEM((1,), jnp.float32),
            dma((10,)),
            dma((2, 2)),
            dma((2, 2)),
            dma((2, n_pieces)),
            dma((2, n_pieces)),
            dma((2, n_pieces)),
            dma((2, n_pieces)),
            dma((3, n_chunks)),
            dma((3, n_chunks)),
            *partner,
        ],
        compiler_params=pltpu.CompilerParams(
            collective_id=level, has_side_effects=True, vmem_limit_bytes=44 << 20
        ),
        cost_estimate=pl.CostEstimate(
            flops=12 * rows * width * units,
            bytes_accessed=2 * (6 * width * units + 2 * seq * width),
            transcendentals=rows * units,
        ),
        name=f"round_level_{level}",
    )(count, round_index, rate, x, g, w_gate, w_up, w_down)
    return write_out(*mixed)


def write_kernel(gate, up, down, out_gate, out_up, out_down, sem):
    copies = [
        pltpu.make_async_copy(src, dst, sem.at[i])
        for i, (src, dst) in enumerate(((gate, out_gate), (up, out_up), (down, out_down)))
    ]
    for copy in copies:
        copy.start()
    for copy in copies:
        copy.wait()


def write_out(*arrays):
    return pl.pallas_call(
        write_kernel,
        out_shape=[jax.ShapeDtypeStruct(a.shape, a.dtype) for a in arrays],
        in_specs=[pl.BlockSpec(memory_space=pltpu.VMEM)] * 3,
        out_specs=[pl.BlockSpec(memory_space=pltpu.HBM)] * 3,
        scratch_shapes=[pltpu.SemaphoreType.DMA((3,))],
        compiler_params=pltpu.CompilerParams(vmem_limit_bytes=16 << 20),
        name="write_out",
    )(*arrays)


def per_device(inputs, upstream, counts, round_index, rates, gate_weight, up_weight, down_weight):
    levels = lax.axis_size("node").bit_length() - 1
    mixed = lax.switch(
        lax.rem(round_index[0], levels),
        [functools.partial(one_level, level, level == levels - 1) for level in range(levels)],
        counts,
        round_index,
        rates,
        inputs[0],
        upstream[0],
        gate_weight[0],
        up_weight[0],
        down_weight[0],
    )
    return tuple(m[None] for m in mixed)


def solution(mesh):
    return jax.shard_map(
        per_device,
        mesh=mesh,
        in_specs=(
            P("node", "shard", None),
            P("node", "shard", None),
            P("node"),
            P(),
            P("node"),
            P("node", None, "shard"),
            P("node", None, "shard"),
            P("node", "shard", None),
        ),
        out_specs=(P("node", None, "shard"), P("node", None, "shard"), P("node", "shard", None)),
        check_vma=False,
    )
```

```python
import functools

import jax
import jax.numpy as jnp
from jax import lax
from jax.experimental import pallas as pl
from jax.experimental.pallas import tpu as pltpu
from jax.sharding import PartitionSpec as P

MESH = pl.DeviceIdType.MESH
CHUNK = 128
BLOCK = 128
PIECE = 64
PARTS = 3

EARLY = ((0, 0, 5), (1, 0, 6), (0, 1, 7))
EARLY_SHARED = ((0, 0, 7),)


def first_late(early):
    return min(blocks for _, _, blocks in early)


def remote(src, dst, send_sem, recv_sem, device):
    return pltpu.make_async_remote_copy(
        src_ref=src,
        dst_ref=dst,
        send_sem=send_sem,
        recv_sem=recv_sem,
        device_id=device,
        device_id_type=MESH,
    )


def round_kernel(
    level,
    early,
    direct,
    count_hbm,
    round_hbm,
    rate_hbm,
    x_hbm,
    g_hbm,
    wg_hbm,
    wu_hbm,
    wd_hbm,
    mixed_gate,
    mixed_up,
    mixed_down,
    raw,
    normed,
    normed_t,
    grad_out,
    w_gate,
    w_up,
    w_down,
    d_both,
    hidden,
    own_gate,
    own_up,
    own_down,
    got_gate,
    got_up,
    got_down,
    count_ref,
    round_ref,
    rate_ref,
    local_sem,
    near_send,
    near_recv,
    far_send,
    far_recv,
    relay_send,
    relay_recv,
    chunk_send,
    chunk_recv,
    passing,
    theirs,
    partial,
    late,
    their_late,
    scalars,
    their_scalars,
    slot_send,
    slot_recv,
    across_send,
    across_recv,
    pass_send,
    pass_recv,
    late_send,
    late_recv,
    scalar_send,
    scalar_recv,
):
    node, shard = lax.axis_index("node"), lax.axis_index("shard")
    core, chip = lax.rem(shard, 2), shard // 2
    near = (node, chip * 2 + 1 - core)
    far = (node, (1 - chip) * 2 + core)
    stride = 1 << level
    other = node + (1 - 2 * lax.rem(node // stride, 2)) * stride
    peer, cross = (other, shard), (other, far[1])
    n_blocks = raw.shape[1]
    width = normed.shape[1]
    n_chunks = own_gate.shape[0]

    def load(i, src, dst):
        return pltpu.make_async_copy(src, dst, local_sem.at[i])

    def rows_of(h):
        return pl.ds(h * BLOCK, BLOCK)

    slot_loads = [
        load(kind * 2 + h, src.at[rows_of(h)], raw.at[kind, h])
        for h in range(2)
        for kind, src in enumerate((x_hbm, g_hbm))
    ]
    other_loads = [
        load(4, wg_hbm, w_gate),
        load(5, wu_hbm, w_up),
        load(6, wd_hbm, w_down),
        load(7, count_hbm, count_ref),
        load(8, round_hbm, round_ref),
        load(9, rate_hbm, rate_ref),
    ]
    for copy in slot_loads:
        copy.start()

    barrier = pltpu.get_barrier_semaphore()
    group = (near, far, peer, cross) if direct else (near, far, peer)
    for device in group:
        pl.semaphore_signal(barrier, inc=1, device_id=device, device_id_type=MESH)
    pl.semaphore_wait(barrier, len(group))

    n_pieces = n_blocks - 4
    per_block = BLOCK // PIECE
    head, tail = pl.ds(0, PIECE), pl.ds(PIECE, PIECE)

    def own_piece(kind, i):
        start = pl.multiple_of((i % per_block) * PIECE, PIECE)
        return raw.at[kind, i // per_block, pl.ds(start, PIECE)]

    def to_near(kind, h):
        return remote(
            raw.at[kind, h], raw.at[kind, 2 + h], near_send.at[kind, h], near_recv.at[kind, h], near
        )

    def to_far(kind, i):
        return remote(
            own_piece(kind, i),
            raw.at[kind, 4 + i, head],
            far_send.at[kind, i],
            far_recv.at[kind, i],
            far,
        )

    def relay(kind, i):
        return remote(
            raw.at[kind, 4 + i, head],
            raw.at[kind, 4 + i, tail],
            relay_send.at[kind, i],
            relay_recv.at[kind, i],
            near,
        )

    both = [(kind, h) for h in range(2) for kind in range(2)]
    pieces = [(kind, i) for i in range(n_pieces) for kind in range(2)]
    pairs = ((own_gate, got_gate), (own_up, got_up), (own_down, got_down))
    first = first_late(early)
    skipped = first - 4
    n_late = n_pieces - skipped

    def to_other(j):
        return remote(
            own_piece(0, j + skipped),
            theirs.at[0, j, head] if direct else passing.at[j],
            slot_send.at[j],
            slot_recv.at[j],
            cross if direct else peer,
        )

    def across(j):
        return remote(
            passing.at[j], theirs.at[0, j, head], across_send.at[j], across_recv.at[j], far
        )

    def pass_on(j):
        return remote(
            theirs.at[0, j, head], theirs.at[0, j, tail], pass_send.at[j], pass_recv.at[j], near
        )

    def late_copy(item, j):
        rows = pl.ds(pl.multiple_of(j * BLOCK, BLOCK), BLOCK)
        return remote(
            late.at[item, rows],
            their_late.at[item, rows],
            late_send.at[item, j],
            late_recv.at[item, j],
            peer,
        )

    def early_copy(item, at=None):
        k, c, _ = early[item]
        mine, got = partial.at[item], pairs[k][1].at[c]
        if at is not None:
            mine, got = mine.at[at], got.at[at]
        return remote(mine, got, chunk_send.at[k, c], chunk_recv.at[k, c], peer)

    scalar_copy = remote(scalars, their_scalars, scalar_send.at[0], scalar_recv.at[0], peer)

    for h in range(2):
        for kind in range(2):
            slot_loads[2 * h + kind].wait()
        for i in range(h * per_block, (h + 1) * per_block):
            for kind in range(2):
                to_far(kind, i).start()
            if i >= skipped:
                to_other(i - skipped).start()
    for copy in other_loads:
        copy.start()
    for kind, h in both:
        to_near(kind, h).start()
    for copy in other_loads:
        copy.wait()

    decay = 250.0 / (250.0 + jnp.full((8, 128), round_ref[0], jnp.int32).astype(jnp.float32))
    step = jnp.max(rate_ref[0] * decay)
    count = count_ref[0].astype(jnp.float32)
    scalars[...] = rate_ref[0] * decay

    def prepare(blocks, block, count):
        to = pl.ds(pl.multiple_of(block * BLOCK, BLOCK), BLOCK)
        floats = blocks[0, block].astype(jnp.float32)
        scale = lax.rsqrt(jnp.mean(floats * floats, -1, keepdims=True) + 1e-06)
        value = (floats * scale).astype(jnp.bfloat16)
        normed[to] = value
        normed_t[:, to] = value.T
        if count is None:
            return
        for half, rest in ((0, 2), (1, 3)):
            slot = lax.bitwise_xor(shard, jnp.where(block < 4, block // 2, rest))
            live = jnp.where(slot.astype(jnp.float32) < count, 1.0, 0.0)
            start = pl.multiple_of(block * BLOCK + half * PIECE, PIECE)
            grad_out[pl.ds(start, PIECE)] = (
                blocks[1, block, half * PIECE : (half + 1) * PIECE].astype(jnp.float32) * live
            ).astype(jnp.bfloat16)

    def units_of(c):
        return pl.ds(pl.multiple_of(c * CHUNK, CHUNK), CHUNK)

    def own_weights(c):
        units = units_of(c)
        return w_gate.at[:, units], w_up.at[:, units], w_down.at[units]

    def forward(c, block):
        gate_weight, up_weight, down_weight = own_weights(c)
        buffer = lax.rem(c, 2)
        at = pl.ds(pl.multiple_of(block * BLOCK, BLOCK), BLOCK)
        n = normed[at]
        gate = jnp.dot(n, gate_weight[...], preferred_element_type=jnp.float32)
        up = jnp.dot(n, up_weight[...], preferred_element_type=jnp.float32)
        back = lax.dot_general(
            grad_out[at],
            down_weight[...],
            (((1,), (1,)), ((), ())),
            preferred_element_type=jnp.float32,
        )
        k = 0.7978845608028654
        square = gate * gate
        t = jnp.tanh(gate * (k + (k * 0.044715) * square))
        half = 0.5 + 0.5 * t
        act = gate * half
        slope = half + (0.5 * gate) * (1.0 - t * t) * (k + (3.0 * k * 0.044715) * square)
        hidden[buffer, at] = (act * up).astype(jnp.bfloat16)
        d_both[buffer, at, :CHUNK] = (back * up * slope).astype(jnp.bfloat16)
        d_both[buffer, at, CHUNK:] = (back * act).astype(jnp.bfloat16)

    part = width // PARTS

    def part_of(b):
        return pl.ds(pl.multiple_of(b * part, part), part)

    def send_early(item):
        k, c, blocks = early[item]
        weight = own_weights(c)[k]
        rows = blocks * BLOCK

        @pl.loop(0, width // BLOCK)
        def _(b):
            at = pl.ds(pl.multiple_of(b * BLOCK, BLOCK), BLOCK)
            grad = jnp.dot(
                normed_t[at, :rows],
                d_both[c, :rows, k * CHUNK : (k + 1) * CHUNK],
                preferred_element_type=jnp.float32,
            )
            partial[item, at] = (weight[at].astype(jnp.float32) - step * grad).astype(
                jnp.bfloat16
            )
            early_copy(item, at).start()

    def send_late(item, block):
        k, c, _ = early[item]
        at = pl.ds(pl.multiple_of(block * BLOCK, BLOCK), BLOCK)
        to = pl.ds(pl.multiple_of((block - first) * BLOCK, BLOCK), BLOCK)
        late[item, to] = d_both[c, at, k * CHUNK : (k + 1) * CHUNK]
        late_copy(item, block - first).start()

    ahead = 1 + max(c for _, c, _ in early)

    @pl.loop(0, n_blocks)
    def _(block):
        @pl.when(block == 2)
        def _():
            for kind, h in both:
                to_near(kind, h).wait_recv()

        @pl.when(block >= 4)
        def _():
            for kind in range(2):
                to_far(kind, block - 4).wait_recv()
                relay(kind, block - 4).start()
            for kind in range(2):
                relay(kind, block - 4).wait_recv()

        prepare(raw, block, count)
        for c in range(ahead):
            forward(c, block)
            items = [(item, blocks) for item, (_, chunk, blocks) in enumerate(early) if chunk == c]
            for item, blocks in items:
                pl.when(block >= blocks)(functools.partial(send_late, item, block))
            for item, blocks in items:
                pl.when(block == blocks - 1)(functools.partial(send_early, item))

    scalar_copy.start()
    if not direct:
        for j in range(n_late):
            to_other(j).wait_recv()
            across(j).start()

    def sent(k, c, at=None):
        mine, other = (ref.at[c] if at is None else ref.at[c, at] for ref in pairs[k])
        return remote(mine, other, chunk_send.at[k, c], chunk_recv.at[k, c], peer)

    def if_late(k, c, act):
        chunks = [chunk for matrix, chunk, _ in early if matrix == k]
        if chunks:
            pl.when(c > max(chunks))(act)
        else:
            act()

    @pl.loop(0, n_chunks)
    def _(c):
        gate_weight, up_weight, down_weight = own_weights(c)
        buffer = lax.rem(c, 2)

        hidden_t = hidden[buffer].T

        @pl.loop(0, PARTS)
        def _(b):
            at = part_of(b)
            grad = jnp.dot(normed_t[at], d_both[buffer], preferred_element_type=jnp.float32)
            own_gate[c, at] = (
                gate_weight[at].astype(jnp.float32) - step * grad[:, :CHUNK]
            ).astype(jnp.bfloat16)
            own_up[c, at] = (
                up_weight[at].astype(jnp.float32) - step * grad[:, CHUNK:]
            ).astype(jnp.bfloat16)
            for k in range(2):
                if_late(k, c, lambda: sent(k, c, at).start())

        @pl.loop(0, PARTS)
        def _(b):
            at = part_of(b)
            grad = jnp.dot(hidden_t, grad_out[:, at], preferred_element_type=jnp.float32)
            own_down[c, :, at] = (
                down_weight[:, at].astype(jnp.float32) - step * grad
            ).astype(jnp.bfloat16)

        sent(2, c).start()

        @pl.when(c < n_chunks - ahead)
        def _():
            @pl.loop(0, n_blocks)
            def _(block):
                forward(c + ahead, block)

    for j in range(n_late):
        (to_other if direct else across)(j).wait_recv()
        pass_on(j).start()
    for item, (_, _, blocks) in enumerate(early):
        early_copy(item).wait_recv()
        for j in range(n_late):
            if first + j >= blocks:
                late_copy(item, j).wait_recv()
            else:
                their_late[item, j * BLOCK : (j + 1) * BLOCK] = jnp.zeros(
                    (BLOCK, CHUNK), jnp.bfloat16
                )
    scalar_copy.wait_recv()
    for j in range(n_late):
        pass_on(j).wait_recv()
    their_step = jnp.max(their_scalars[...])

    @pl.loop(0, n_late)
    def _(j):
        prepare(theirs, j, None)

    for item, (k, c, _) in enumerate(early):
        result = pairs[k][1].at[c]

        @pl.loop(0, PARTS)
        def _(b):
            at = part_of(b)
            grad = jnp.dot(
                normed_t[at, : n_late * BLOCK],
                their_late[item],
                preferred_element_type=jnp.float32,
            )
            result[at] = (result[at].astype(jnp.float32) - their_step * grad).astype(jnp.bfloat16)

    def average(mine, theirs):
        return (0.5 * (mine.astype(jnp.float32) + theirs.astype(jnp.float32))).astype(jnp.bfloat16)

    for kind, h in both:
        to_near(kind, h).wait_send()
    for kind, i in pieces:
        to_far(kind, i).wait_send()
        relay(kind, i).wait_send()
    scalar_copy.wait_send()
    for j in range(n_late):
        to_other(j).wait_send()
        if not direct:
            across(j).wait_send()
        pass_on(j).wait_send()
    for item, (_, _, blocks) in enumerate(early):
        early_copy(item).wait_send()
        for j in range(blocks - first, n_late):
            late_copy(item, j).wait_send()

    @pl.loop(0, n_chunks)
    def _(c):
        units = units_of(c)

        if_late(0, c, lambda: sent(0, c).wait_recv())
        mixed_gate[:, units] = average(own_gate[c], got_gate[c])
        if_late(1, c, lambda: sent(1, c).wait_recv())
        mixed_up[:, units] = average(own_up[c], got_up[c])
        sent(2, c).wait_recv()
        mixed_down[units] = average(own_down[c], got_down[c])

        @pl.when(c < n_chunks - 1)
        def _():
            if_late(0, c, lambda: sent(0, c).wait_send())
            if_late(1, c, lambda: sent(1, c).wait_send())
            sent(2, c).wait_send()

    for k in range(3):
        sent(k, n_chunks - 1).wait_send()


def one_level(level, shared, count, round_index, rate, x, g, w_gate, w_up, w_down):
    seq, width = x.shape
    units = w_gate.shape[1]
    n_chunks, rows = units // CHUNK, 4 * seq
    bf16 = jnp.bfloat16
    hbm = pl.BlockSpec(memory_space=pltpu.HBM)
    vmem = pl.BlockSpec(memory_space=pltpu.VMEM)
    dma = pltpu.SemaphoreType.DMA
    across = pltpu.VMEM((n_chunks, width, CHUNK), bf16)
    along = pltpu.VMEM((n_chunks, CHUNK, width), bf16)
    raw = pltpu.VMEM((2, rows // BLOCK, BLOCK, width), bf16)
    n_pieces = seq // PIECE
    early = EARLY_SHARED if shared else EARLY
    n_late = 4 + n_pieces - first_late(early)
    late = pltpu.VMEM((len(early), n_late * BLOCK, CHUNK), bf16)
    scalar = pltpu.VMEM((8, 128), jnp.float32)
    partner = [
        pltpu.VMEM((n_late, PIECE, width), bf16),
        pltpu.VMEM((1, n_late, BLOCK, width), bf16),
        pltpu.VMEM((len(early), width, CHUNK), bf16),
        late,
        late,
        scalar,
        scalar,
    ]
    partner += [dma((n_late,))] * 6 + [dma((len(early), n_late))] * 2 + [dma((1,))] * 2
    mixed = pl.pallas_call(
        functools.partial(round_kernel, level, early, shared),
        out_shape=[pltpu.VMEM(w.shape, bf16) for w in (w_gate, w_up, w_down)],
        in_specs=[hbm] * 8,
        out_specs=[vmem] * 3,
        scratch_shapes=[
            raw,
            pltpu.VMEM((rows, width), bf16),
            pltpu.VMEM((width, rows), bf16),
            pltpu.VMEM((rows, width), bf16),
            pltpu.VMEM(w_gate.shape, bf16),
            pltpu.VMEM(w_up.shape, bf16),
            pltpu.VMEM(w_down.shape, bf16),
            pltpu.VMEM((2, rows, 2 * CHUNK), bf16),
            pltpu.VMEM((2, rows, CHUNK), bf16),
            across,
            across,
            along,
            across,
            across,
            along,
            pltpu.SMEM((1,), jnp.int32),
            pltpu.SMEM((1,), jnp.int32),
            pltpu.SMEM((1,), jnp.float32),
            dma((10,)),
            dma((2, 2)),
            dma((2, 2)),
            dma((2, n_pieces)),
            dma((2, n_pieces)),
            dma((2, n_pieces)),
            dma((2, n_pieces)),
            dma((3, n_chunks)),
            dma((3, n_chunks)),
            *partner,
        ],
        compiler_params=pltpu.CompilerParams(
            collective_id=level, has_side_effects=True, vmem_limit_bytes=44 << 20
        ),
        cost_estimate=pl.CostEstimate(
            flops=12 * rows * width * units,
            bytes_accessed=2 * (6 * width * units + 2 * seq * width),
            transcendentals=rows * units,
        ),
        name=f"round_level_{level}",
    )(count, round_index, rate, x, g, w_gate, w_up, w_down)
    return write_out(*mixed)


def write_kernel(gate, up, down, out_gate, out_up, out_down, sem):
    copies = [
        pltpu.make_async_copy(src, dst, sem.at[i])
        for i, (src, dst) in enumerate(((gate, out_gate), (up, out_up), (down, out_down)))
    ]
    for copy in copies:
        copy.start()
    for copy in copies:
        copy.wait()


def write_out(*arrays):
    return pl.pallas_call(
        write_kernel,
        out_shape=[jax.ShapeDtypeStruct(a.shape, a.dtype) for a in arrays],
        in_specs=[pl.BlockSpec(memory_space=pltpu.VMEM)] * 3,
        out_specs=[pl.BlockSpec(memory_space=pltpu.HBM)] * 3,
        scratch_shapes=[pltpu.SemaphoreType.DMA((3,))],
        compiler_params=pltpu.CompilerParams(vmem_limit_bytes=16 << 20),
        name="write_out",
    )(*arrays)


def per_device(inputs, upstream, counts, round_index, rates, gate_weight, up_weight, down_weight):
    levels = lax.axis_size("node").bit_length() - 1
    mixed = lax.switch(
        lax.rem(round_index[0], levels),
        [functools.partial(one_level, level, level == levels - 1) for level in range(levels)],
        counts,
        round_index,
        rates,
        inputs[0],
        upstream[0],
        gate_weight[0],
        up_weight[0],
        down_weight[0],
    )
    return tuple(m[None] for m in mixed)


def solution(mesh):
    return jax.shard_map(
        per_device,
        mesh=mesh,
        in_specs=(
            P("node", "shard", None),
            P("node", "shard", None),
            P("node"),
            P(),
            P("node"),
            P("node", None, "shard"),
            P("node", None, "shard"),
            P("node", "shard", None),
        ),
        out_specs=(P("node", None, "shard"), P("node", None, "shard"), P("node", "shard", None)),
        check_vma=False,
    )
```
